32 devices in a mesh: gx: 4 (over x, core), gy: 8 (over z, y).
Axes of the slice: x: 2, y: 2, z: 4, core: 2. Of those that a mesh axis runs over, the one named last changes fastest.
Arguments:
- hot_ids: int32 [262144], P(('gx', 'gy')), may hold values from 0 to 2047
- hot_grads: bfloat16 [262144, 128], P(('gx', 'gy')), may hold values from -6 to 6
- cold_grads: bfloat16 [4, 8, 8, 512, 128], P('gx', 'gy'), may hold values from -6 to 6
- cold_slots: int32 [4, 8, 8, 512], P('gx', 'gy'), may hold values from 0 to 2047
- cold_counts: int32 [4, 8, 8], P('gx', 'gy'), may hold values from 1 to 512, as said below
Outputs:
- hot_grad: float32 [2048, 128], replicated
- cold_grad: float32 [4, 16384, 128], P('gx', 'gy')
The draws below stay inside these ranges and needn't reach their ends.
Inputs may be any that keep to these rules, and one draw needn't show every extreme that they name: In each group g, some owner d receives cold_counts[g, s, d] = 512 from every s; loads per owner are skewed.
All inputs are finite; a program needn't handle non-finite values.
Results may differ from the reference program's by a relative error of at most 0.0003.
Values may be sent and summed in bfloat16 or wider, within the bound.
No kernel may reach another device: no remote copies, remote signals or barrier semaphores. Data moves between devices by JAX's collectives and lax.ppermute only.
A program may use at most 64 MiB of HBM per device.

```python
import jax
import jax.numpy as jnp
from jax import lax

D = 128
HOT = 2048
LOOK = 8192
CAP = 512
OWN_ROWS = 2048
LOOKUPS = 262144
N_GX = 4
N_GY = 8


def draw_cold_counts(key, part):
    first = jax.random.fold_in(key, 11)
    second = jax.random.fold_in(key, 12)
    third = jax.random.fold_in(key, 13)
    limits = jax.random.randint(first, (N_GX, 1, N_GY), 1, CAP + 1)
    counts = jax.random.randint(second, (N_GX, N_GY, N_GY), 1, CAP + 1)
    counts = jnp.minimum(counts, limits)
    heavy = jax.random.randint(third, (N_GX, 1, 1), 0, N_GY)
    owners = jnp.arange(N_GY, dtype=jnp.int32)[None, None, :]
    return jnp.where(owners == heavy, CAP, counts).astype(jnp.int32)


def with_ends(values, rng, least, high):
    dims = values.shape
    spot = [jax.random.randint(jax.random.fold_in(rng, axis), (), 0, dims[axis]) for axis in range(len(dims))]
    values = values.at[tuple(spot)].set(least)
    longest = dims.index(max(dims))
    spot[longest] = (spot[longest] + 1) % dims[longest]
    return values.at[tuple(spot)].set(high)


def block_levels(rng, dims, shards, low, top_value):
    def one(dim, blocks):
        steps = jax.random.uniform(jax.random.fold_in(jax.random.fold_in(rng, 6), dim), (blocks,), jnp.float32, low / len(shards), top_value / len(shards))
        return jnp.repeat(jnp.exp(steps), dims[dim] // blocks).reshape((-1,) + (1,) * (len(dims) - dim - 1))

    gain = one(*shards[0])
    for cut in shards[1:]:
        gain = gain * one(*cut)
    return gain


def scatter_about(own_key, shape, spread, bound, split=(), kind=jnp.bfloat16):
    gain = block_levels(own_key, shape, split, -0.22, 0.18) if split else 1.0
    result = jax.random.normal(own_key, shape, jnp.float32) * spread * gain
    return jnp.minimum(jnp.maximum(result, -bound), bound).astype(kind)


def setup_inputs(seed: int = 0) -> dict:
    arg_keys = jax.random.split(jax.random.key(seed), 6)
    hot_ids = with_ends(jax.random.randint(arg_keys[0], (LOOKUPS,), 0, HOT), jax.random.fold_in(arg_keys[0], 1), 0, HOT - 1).astype(jnp.int32)
    hot_grads = scatter_about(arg_keys[1], (LOOKUPS, D), 1.0, 6.0, ((0, 32),))
    cold_grads = scatter_about(arg_keys[2], (N_GX, N_GY, N_GY, CAP, D), 1.0, 6.0, ((0, 4), (1, 8)))
    cold_slots = with_ends(jax.random.randint(arg_keys[3], (N_GX, N_GY, N_GY, CAP), 0, OWN_ROWS), jax.random.fold_in(arg_keys[3], 1), 0, OWN_ROWS - 1).astype(jnp.int32)
    cold_counts = draw_cold_counts(jax.random.fold_in(arg_keys[5], 71), 0)
    return dict(hot_ids=hot_ids, hot_grads=hot_grads, cold_grads=cold_grads, cold_slots=cold_slots, cold_counts=cold_counts)


def reference(hot_ids, hot_grads, cold_grads, cold_slots, cold_counts):
    hot_sum = jax.ops.segment_sum(hot_grads.astype(jnp.float32), hot_ids, num_segments=HOT)
    hot_grad = hot_sum * (HOT / (LOOK * N_GX * N_GY)) ** 0.5
    places = jnp.arange(CAP, dtype=jnp.int32)
    valid = places[None, None, None, :] < cold_counts[..., None]
    payload = jnp.where(valid[..., None], cold_grads, jnp.zeros_like(cold_grads))
    owners = jnp.arange(N_GY, dtype=jnp.int32)[None, None, :, None] * OWN_ROWS
    table_rows = (owners + cold_slots).astype(jnp.int32)

    def one_group(pair):
        rows_data, rows_index = pair
        return jax.ops.segment_sum(rows_data.reshape(-1, D).astype(jnp.float32), rows_index.reshape(-1), num_segments=OWN_ROWS * N_GY)

    cold_grad = lax.map(one_group, (payload, table_rows))
    return hot_grad, cold_grad
```

```python
import functools
import math

import jax
import jax.numpy as jnp
from jax import lax
from jax.experimental import pallas as pl
from jax.experimental.pallas import tpu as pltpu
from jax.sharding import Mesh
from jax.sharding import PartitionSpec as P

HOT = 2048
OWN_ROWS = 2048
LANES = 128
SUB = 8
STEPS = 128.0
TOP = 32600.0
TINY = 2.0**-100


def masked_halves(keep, data_ref, rhs_ref, base, width):
    flags = keep.T
    for j in range(keep.shape[0]):
        rows = pl.ds(base + j * LANES, LANES)
        column = jnp.broadcast_to(flags[:, j : j + 1], (LANES, width)).astype(jnp.bfloat16)
        data = data_ref[pl.ds(j * LANES, LANES), :]
        kept = data * column
        rhs_ref[rows, :width] = kept
        rhs_ref[rows, width:] = data - kept


def onehot_block(row, start, size):
    places = (lax.broadcasted_iota(jnp.int32, (size, LANES), 0) + start).astype(jnp.int16)
    one, zero = jnp.ones((), jnp.bfloat16), jnp.zeros((), jnp.bfloat16)
    parts = [jnp.where(places == row[j : j + 1, :], one, zero) for j in range(row.shape[0])]
    return jnp.concatenate(parts, axis=1)


def hot_kernel(core_ref, ids_ref, data_ref, mine_ref, send_ref, rhs_ref, *, block):
    half, width = mine_ref.shape

    @pl.when(pl.program_id(0) == 0)
    def _():
        mine_ref[...] = jnp.zeros_like(mine_ref)
        send_ref[...] = jnp.zeros_like(send_ref)

    ids = ids_ref[...]
    high = (ids >= half).astype(jnp.int32)
    masked_halves((high == core_ref[0]).astype(jnp.float32), data_ref, rhs_ref, 0, width)
    row = (ids - high * half).astype(jnp.int16)
    rhs = rhs_ref[...]
    for start in range(0, half, block):
        part = jnp.dot(onehot_block(row, start, block), rhs, preferred_element_type=jnp.float32)
        rows = pl.ds(start, block)
        mine_ref[rows, :] += part[:, :width]
        send_ref[rows, :] += part[:, width:]


def hot_sums(core, ids, data, table):
    lookups, width = data.shape
    half = table // 2
    step = math.gcd(lookups, 4096)
    return pl.pallas_call(
        functools.partial(hot_kernel, block=math.gcd(half, 256)),
        grid=(lookups // step,),
        in_specs=[
            pl.BlockSpec(memory_space=pltpu.SMEM),
            pl.BlockSpec((step // LANES, LANES), lambda i: (i, 0)),
            pl.BlockSpec((step, width), lambda i: (i, 0)),
        ],
        out_specs=[pl.BlockSpec((half, width), lambda i: (0, 0))] * 2,
        out_shape=[jax.ShapeDtypeStruct((half, width), jnp.float32)] * 2,
        scratch_shapes=[pltpu.VMEM((step, 2 * width), jnp.bfloat16)],
        cost_estimate=pl.CostEstimate(flops=2 * lookups * table * width, bytes_accessed=2 * lookups * width, transcendentals=0),
        name="hot_sums",
    )(core, ids.reshape(lookups // LANES, LANES), data)


def encode(values):
    rows, width = values.shape
    groups = values.reshape(rows // SUB, SUB, width)
    most = jnp.maximum(jnp.max(jnp.abs(groups), axis=0), TINY)
    code = jnp.ceil(jnp.log2(most) * STEPS) + 1.0
    codes = jnp.round(groups * (jnp.exp2(code * (-1.0 / STEPS)) * TOP)[None])
    return codes.reshape(rows, width), code


def decode(codes, code):
    rows, width = codes.shape
    scale = jnp.exp2(code * (1.0 / STEPS)) * (1.0 / TOP)
    return (codes.reshape(rows // SUB, SUB, width) * scale[None]).reshape(rows, width)


def narrow(values):
    return values.astype(jnp.int32).astype(jnp.int16)


def widen(values):
    return values.astype(jnp.int32).astype(jnp.float32)


def pack_kernel(counts_ref, mine_ref, got_ref, slots_ref, out_ref):
    peers, rows, width = out_ref.shape
    rows -= 2 * SUB
    owners, lines, _ = slots_ref.shape
    places = lax.broadcasted_iota(jnp.int32, (lines, LANES), 0) * LANES + lax.broadcasted_iota(jnp.int32, (lines, LANES), 1)
    for p in range(peers):
        here = pl.ds(p * rows, rows)
        codes, code = encode(mine_ref[here, :] + got_ref[here, :])
        out_ref[p, :rows, :] = narrow(codes)
        d = p % owners
        used = jnp.where(places < counts_ref[d], slots_ref[d], -1)
        if lines < SUB:
            used = jnp.concatenate([used, jnp.full((SUB - lines, LANES), -1, jnp.int32)], axis=0)
        tail = jnp.concatenate([code.astype(jnp.int32), used], axis=0)
        out_ref[p, rows:, :] = tail.astype(jnp.int16)


def pack(mine, got, slots, counts, peers):
    half, width = mine.shape
    whole = pl.BlockSpec(memory_space=pltpu.VMEM)
    return pl.pallas_call(
        pack_kernel,
        in_specs=[pl.BlockSpec(memory_space=pltpu.SMEM), whole, whole, whole],
        out_specs=whole,
        out_shape=jax.ShapeDtypeStruct((peers, half // peers + 2 * SUB, width), jnp.int16),
        cost_estimate=pl.CostEstimate(flops=half * width * 8, bytes_accessed=half * width * 10, transcendentals=0),
        name="pack",
    )(counts, mine, got, slots)


def add_kernel(got_ref, out_ref, *, factor):
    peers, rows, width = got_ref.shape
    rows -= 2 * SUB
    total = jnp.zeros((rows, width), jnp.float32)
    for p in range(peers):
        tail = widen(got_ref[p, rows:, :])
        total += decode(widen(got_ref[p, :rows, :]), tail[:SUB])
    codes, code = encode(total * factor)
    packed = jnp.concatenate([narrow(codes), narrow(jnp.concatenate([code, code], axis=0))], axis=0)
    for p in range(peers):
        out_ref[p] = packed


def add(got, factor):
    whole = pl.BlockSpec(memory_space=pltpu.VMEM)
    return pl.pallas_call(
        functools.partial(add_kernel, factor=factor),
        in_specs=[whole],
        out_specs=whole,
        out_shape=jax.ShapeDtypeStruct(got.shape, jnp.int16),
        cost_estimate=pl.CostEstimate(flops=got.size * 8, bytes_accessed=got.size * 4, transcendentals=0),
        name="add",
    )(got)


def unpack_kernel(core_ref, mine_ref, other_ref, out_ref):
    peers, rows, width = mine_ref.shape
    rows -= 2 * SUB
    core = core_ref[0]
    for ref, side in ((mine_ref, core), (other_ref, 1 - core)):
        for p in range(peers):
            tail = widen(ref[p, rows:, :])
            start = pl.multiple_of(side * (peers * rows) + p * rows, SUB)
            out_ref[pl.ds(start, rows), :] = decode(widen(ref[p, :rows, :]), tail[:SUB])


def unpack(core, mine, other, table):
    peers, rows, width = mine.shape
    whole = pl.BlockSpec(memory_space=pltpu.VMEM)
    return pl.pallas_call(
        unpack_kernel,
        in_specs=[pl.BlockSpec(memory_space=pltpu.SMEM), whole, whole],
        out_specs=whole,
        out_shape=jax.ShapeDtypeStruct((table, width), jnp.float32),
        cost_estimate=pl.CostEstimate(flops=table * width * 4, bytes_accessed=table * width * 6, transcendentals=0),
        name="unpack",
    )(core, mine, other)


def cold_kernel(group_ref, slots_ref, data_ref, out_ref, rhs_ref, row_ref, *, block, at, lines):
    owners, capacity, width = data_ref.shape
    half = out_ref.shape[0] // 2
    for s in range(owners):
        slots = slots_ref[s, at:, :].astype(jnp.int32)[SUB : SUB + lines]
        high = (slots >= half).astype(jnp.int32)
        masked_halves((high == 0).astype(jnp.float32), data_ref.at[s], rhs_ref, s * capacity, width)
        row_ref[pl.ds(s * lines, lines), :] = slots - high * half
    row = row_ref[...].astype(jnp.int16)
    rhs = rhs_ref[...]
    for start in range(0, half, block):
        part = jnp.dot(onehot_block(row, start, block), rhs, preferred_element_type=jnp.float32)
        out_ref[pl.ds(start, block), :] = part[:, :width]
        out_ref[pl.ds(half + start, block), :] = part[:, width:]


def cold_sums(group, got, data, table):
    owners, capacity, width = data.shape
    lines = capacity // LANES
    rows = got.shape[1]
    return pl.pallas_call(
        functools.partial(cold_kernel, block=math.gcd(table // 2, 256), at=rows - 2 * SUB, lines=lines),
        grid_spec=pltpu.PrefetchScalarGridSpec(
            num_scalar_prefetch=1,
            grid=(1,),
            in_specs=[
                pl.BlockSpec((owners, rows, LANES), lambda i, group: (group[0], 0, 0)),
                pl.BlockSpec((owners, capacity, width), lambda i, group: (0, 0, 0)),
            ],
            out_specs=pl.BlockSpec((table, width), lambda i, group: (0, 0)),
            scratch_shapes=[
                pltpu.VMEM((owners * capacity, 2 * width), jnp.bfloat16),
                pltpu.VMEM((owners * lines, LANES), jnp.int32),
            ],
        ),
        out_shape=jax.ShapeDtypeStruct((table, width), jnp.float32),
        cost_estimate=pl.CostEstimate(flops=2 * owners * capacity * table * width, bytes_accessed=2 * owners * capacity * width, transcendentals=0),
        name="cold_sums",
    )(group, got, data)


def per_device(hot_ids, hot_grads, cold_grads, cold_slots, cold_counts):
    groups, owners = lax.axis_size("chip"), lax.axis_size("gy")
    peers = groups * owners
    everyone = ("chip", "gy")
    core = lax.axis_index("core").astype(jnp.int32).reshape(1)
    chip = lax.axis_index("chip").astype(jnp.int32).reshape(1)
    swap = [(0, 1), (1, 0)]
    factor = (HOT / (hot_ids.shape[0] * peers * 2)) ** 0.5

    capacity, width = cold_grads.shape[3:]
    blocks = cold_grads.reshape(owners, capacity, width)
    slots = cold_slots.reshape(owners, capacity // LANES, LANES)
    cold_rows = lax.all_to_all(blocks, "gy", split_axis=0, concat_axis=0, tiled=True)

    mine, send = hot_sums(core, hot_ids, hot_grads, HOT)
    got = lax.ppermute(send, "core", swap)
    packed = pack(mine, got, slots, cold_counts.reshape(owners), peers)
    parts = lax.all_to_all(packed, everyone, split_axis=0, concat_axis=0, tiled=True)
    summed = add(parts, factor)
    all_rows = lax.all_to_all(summed, everyone, split_axis=0, concat_axis=0, tiled=True)
    others = lax.ppermute(all_rows, "core", swap)
    hot_grad = unpack(core, all_rows, others, HOT)

    cold_grad = cold_sums(chip, parts, cold_rows, OWN_ROWS)
    return hot_grad, cold_grad.reshape(1, OWN_ROWS, width)


def solution(mesh):
    wide, owners = mesh.devices.shape
    split = Mesh(mesh.devices.reshape(wide // 2, 2, owners), ("chip", "core", "gy"))
    every = ("chip", "core", "gy")
    gx = ("chip", "core")
    return jax.shard_map(
        per_device,
        mesh=split,
        in_specs=(
            P(every),
            P(every, None),
            P(gx, "gy", None, None, None),
            P(gx, "gy", None, None),
            P(gx, "gy", None),
        ),
        out_specs=(P(), P(gx, "gy", None)),
        check_vma=False,
    )
```

```python
import functools
import math

import jax
import jax.numpy as jnp
from jax import lax
from jax.experimental import pallas as pl
from jax.experimental.pallas import tpu as pltpu
from jax.sharding import Mesh
from jax.sharding import PartitionSpec as P


HOT = 2048
OWN_ROWS = 2048
LANES = 128
SUB = 8
STEPS = 128.0
TOP = 32600.0
TINY = 2.0**-100
ROOM = pltpu.CompilerParams(vmem_limit_bytes=20 * 2**20)


def masked_halves(keep, data_ref, rhs_ref, base, width):
    flags = keep.T
    for j in range(keep.shape[0]):
        rows = pl.ds(base + j * LANES, LANES)
        column = jnp.broadcast_to(flags[:, j : j + 1], (LANES, width)).astype(jnp.bfloat16)
        data = data_ref[pl.ds(j * LANES, LANES), :]
        kept = data * column
        rhs_ref[rows, :width] = kept
        rhs_ref[rows, width:] = data - kept


def onehot_block(row, start, size):
    places = (lax.broadcasted_iota(jnp.int32, (size, LANES), 0) + start).astype(jnp.int16)
    one, zero = jnp.ones((), jnp.bfloat16), jnp.zeros((), jnp.bfloat16)
    parts = [jnp.where(places == row[j : j + 1, :], one, zero) for j in range(row.shape[0])]
    return jnp.concatenate(parts, axis=1)


def hot_kernel(core_ref, ids_ref, data_ref, mine_ref, send_ref, rhs_ref, *, block):
    half, width = mine_ref.shape

    @pl.when(pl.program_id(0) == 0)
    def _():
        mine_ref[...] = jnp.zeros_like(mine_ref)
        send_ref[...] = jnp.zeros_like(send_ref)

    ids = ids_ref[...]
    high = (ids >= half).astype(jnp.int32)
    masked_halves((high == core_ref[0]).astype(jnp.float32), data_ref, rhs_ref, 0, width)
    row = (ids - high * half).astype(jnp.int16)
    rhs = rhs_ref[...]
    for start in range(0, half, block):
        part = jnp.dot(onehot_block(row, start, block), rhs, preferred_element_type=jnp.float32)
        rows = pl.ds(start, block)
        mine_ref[rows, :] += part[:, :width]
        send_ref[rows, :] += part[:, width:]


def hot_sums(core, ids, data, table):
    lookups, width = data.shape
    half = table // 2
    step = math.gcd(lookups, 4096)
    return pl.pallas_call(
        functools.partial(hot_kernel, block=math.gcd(half, 256)),
        grid=(lookups // step,),
        in_specs=[
            pl.BlockSpec(memory_space=pltpu.SMEM),
            pl.BlockSpec((step // LANES, LANES), lambda i: (i, 0)),
            pl.BlockSpec((step, width), lambda i: (i, 0)),
        ],
        out_specs=[pl.BlockSpec((half, width), lambda i: (0, 0))] * 2,
        out_shape=[jax.ShapeDtypeStruct((half, width), jnp.float32)] * 2,
        scratch_shapes=[pltpu.VMEM((step, 2 * width), jnp.bfloat16)],
        cost_estimate=pl.CostEstimate(flops=2 * lookups * table * width, bytes_accessed=2 * lookups * width, transcendentals=0),
        compiler_params=ROOM,
        name="hot_sums",
    )(core, ids.reshape(lookups // LANES, LANES), data)


def encode(values):
    rows, width = values.shape
    groups = values.reshape(rows // SUB, SUB, width)
    most = jnp.maximum(jnp.max(jnp.abs(groups), axis=0), TINY)
    code = jnp.ceil(jnp.log2(most) * STEPS) + 1.0
    codes = jnp.round(groups * (jnp.exp2(code * (-1.0 / STEPS)) * TOP)[None])
    return codes.reshape(rows, width), code


def decode(codes, code):
    rows, width = codes.shape
    scale = jnp.exp2(code * (1.0 / STEPS)) * (1.0 / TOP)
    return (codes.reshape(rows // SUB, SUB, width) * scale[None]).reshape(rows, width)


def narrow(values):
    return values.astype(jnp.int32).astype(jnp.int16)


def widen(values):
    return values.astype(jnp.int32).astype(jnp.float32)


def pack_kernel(counts_ref, mine_ref, got_ref, slots_ref, out_ref):
    peers, rows, _ = out_ref.shape
    rows -= 2 * SUB
    owners, lines, _ = slots_ref.shape
    places = lax.broadcasted_iota(jnp.int32, (lines, LANES), 0) * LANES + lax.broadcasted_iota(jnp.int32, (lines, LANES), 1)
    for p in range(peers):
        here = pl.ds(p * rows, rows)
        codes, code = encode(mine_ref[here, :] + got_ref[here, :])
        out_ref[p, :rows, :] = narrow(codes)
        d = p % owners
        used = jnp.where(places < counts_ref[d], slots_ref[d], -1)
        if lines < SUB:
            used = jnp.concatenate([used, jnp.full((SUB - lines, LANES), -1, jnp.int32)], axis=0)
        tail = jnp.concatenate([code.astype(jnp.int32), used], axis=0)
        out_ref[p, rows:, :] = tail.astype(jnp.int16)


def pack(mine, got, slots, counts, peers):
    half, width = mine.shape
    whole = pl.BlockSpec(memory_space=pltpu.VMEM)
    return pl.pallas_call(
        pack_kernel,
        in_specs=[pl.BlockSpec(memory_space=pltpu.SMEM), whole, whole, whole],
        out_specs=whole,
        out_shape=jax.ShapeDtypeStruct((peers, half // peers + 2 * SUB, width), jnp.int16),
        cost_estimate=pl.CostEstimate(flops=half * width * 8, bytes_accessed=half * width * 10, transcendentals=0),
        compiler_params=ROOM,
        name="pack",
    )(counts, mine, got, slots)


def add_kernel(got_ref, out_ref, *, factor):
    peers, rows, width = got_ref.shape
    rows -= 2 * SUB
    total = jnp.zeros((rows, width), jnp.float32)
    for p in range(peers):
        tail = widen(got_ref[p, rows:, :])
        total += decode(widen(got_ref[p, :rows, :]), tail[:SUB])
    codes, code = encode(total * factor)
    packed = jnp.concatenate([narrow(codes), narrow(jnp.concatenate([code, code], axis=0))], axis=0)
    for p in range(peers):
        out_ref[p] = packed


def add(got, factor):
    whole = pl.BlockSpec(memory_space=pltpu.VMEM)
    return pl.pallas_call(
        functools.partial(add_kernel, factor=factor),
        in_specs=[whole],
        out_specs=whole,
        out_shape=jax.ShapeDtypeStruct(got.shape, jnp.int16),
        cost_estimate=pl.CostEstimate(flops=got.size * 8, bytes_accessed=got.size * 4, transcendentals=0),
        compiler_params=ROOM,
        name="add",
    )(got)


def unpack_kernel(core_ref, mine_ref, other_ref, out_ref):
    peers, rows, _ = mine_ref.shape
    rows -= 2 * SUB
    core = core_ref[0]
    for ref, side in ((mine_ref, core), (other_ref, 1 - core)):
        for p in range(peers):
            tail = widen(ref[p, rows:, :])
            start = pl.multiple_of(side * (peers * rows) + p * rows, SUB)
            out_ref[pl.ds(start, rows), :] = decode(widen(ref[p, :rows, :]), tail[:SUB])


def unpack(core, mine, other, table):
    _, _, width = mine.shape
    whole = pl.BlockSpec(memory_space=pltpu.VMEM)
    return pl.pallas_call(
        unpack_kernel,
        in_specs=[pl.BlockSpec(memory_space=pltpu.SMEM), whole, whole],
        out_specs=whole,
        out_shape=jax.ShapeDtypeStruct((table, width), jnp.float32),
        cost_estimate=pl.CostEstimate(flops=table * width * 4, bytes_accessed=table * width * 6, transcendentals=0),
        compiler_params=ROOM,
        name="unpack",
    )(core, mine, other)


def partner(me, step, count):
    if count & (count - 1):
        return (me - step) % count, (me + step) % count
    return me ^ step, me ^ step


def cold_kernel(place_ref, slots_ref, own_ref, *refs, block, at, lines):
    moved, (out_ref, rhs_ref, row_ref) = refs[:-3], refs[-3:]
    _, capacity, width = own_ref.shape
    owners = len(moved) + 1
    half = out_ref.shape[0] // 2
    for step, ref in enumerate((own_ref.at[0], *moved)):
        source, _ = partner(place_ref[1], step, owners)
        slots = slots_ref[source, at:, :].astype(jnp.int32)[SUB : SUB + lines]
        high = (slots >= half).astype(jnp.int32)
        masked_halves((high == 0).astype(jnp.float32), ref, rhs_ref, step * capacity, width)
        row_ref[pl.ds(step * lines, lines), :] = slots - high * half
    row = row_ref[...].astype(jnp.int16)
    rhs = rhs_ref[...]
    for start in range(0, half, block):
        part = jnp.dot(onehot_block(row, start, block), rhs, preferred_element_type=jnp.float32)
        out_ref[pl.ds(start, block), :] = part[:, :width]
        out_ref[pl.ds(half + start, block), :] = part[:, width:]


def cold_sums(place, got, own, moved, table):
    owners, capacity, width = own.shape
    lines = capacity // LANES
    rows = got.shape[1]
    return pl.pallas_call(
        functools.partial(cold_kernel, block=math.gcd(table // 2, 256), at=rows - 2 * SUB, lines=lines),
        grid_spec=pltpu.PrefetchScalarGridSpec(
            num_scalar_prefetch=1,
            grid=(1,),
            in_specs=[
                pl.BlockSpec((owners, rows, LANES), lambda i, place: (place[0], 0, 0)),
                pl.BlockSpec((1, capacity, width), lambda i, place: (place[1], 0, 0)),
            ]
            + [pl.BlockSpec((capacity, width), lambda i, place: (0, 0))] * len(moved),
            out_specs=pl.BlockSpec((table, width), lambda i, place: (0, 0)),
            scratch_shapes=[
                pltpu.VMEM((owners * capacity, 2 * width), jnp.bfloat16),
                pltpu.VMEM((owners * lines, LANES), jnp.int32),
            ],
        ),
        out_shape=jax.ShapeDtypeStruct((table, width), jnp.float32),
        cost_estimate=pl.CostEstimate(flops=2 * owners * capacity * table * width, bytes_accessed=2 * owners * capacity * width, transcendentals=0),
        compiler_params=ROOM,
        name="cold_sums",
    )(place, got, own, *moved)


def per_device(hot_ids, hot_grads, cold_grads, cold_slots, cold_counts):
    groups, owners = lax.axis_size("chip"), lax.axis_size("gy")
    peers = groups * owners
    everyone = ("chip", "gy")
    core = lax.axis_index("core").astype(jnp.int32).reshape(1)
    chip, owner = lax.axis_index("chip"), lax.axis_index("gy")
    place = jnp.stack([chip, owner]).astype(jnp.int32)
    swap = [(0, 1), (1, 0)]
    factor = (HOT / (hot_ids.shape[0] * peers * 2)) ** 0.5

    capacity, width = cold_grads.shape[3:]
    blocks = cold_grads.reshape(owners, capacity, width)
    slots = cold_slots.reshape(owners, capacity // LANES, LANES)
    moved = []
    for step in range(1, owners):
        pairs = [(i, partner(i, step, owners)[1]) for i in range(owners)]
        block = lax.dynamic_index_in_dim(blocks, partner(owner, step, owners)[1], 0, keepdims=False)
        moved.append(lax.ppermute(block, "gy", pairs))
    mine, send = hot_sums(core, hot_ids, hot_grads, HOT)
    got = lax.ppermute(send, "core", swap)
    packed = pack(mine, got, slots, cold_counts.reshape(owners), peers)
    parts = lax.all_to_all(packed, everyone, split_axis=0, concat_axis=0, tiled=True)
    summed = add(parts, factor)
    all_rows = lax.all_to_all(summed, everyone, split_axis=0, concat_axis=0, tiled=True)
    cold_grad = cold_sums(place, parts, blocks, moved, OWN_ROWS)
    others = lax.ppermute(all_rows, "core", swap)
    hot_grad = unpack(core, all_rows, others, HOT)
    return hot_grad, cold_grad.reshape(1, OWN_ROWS, width)


def solution(mesh):
    wide, owners = mesh.devices.shape
    split = Mesh(mesh.devices.reshape(wide // 2, 2, owners), ("chip", "core", "gy"))
    every = ("chip", "core", "gy")
    gx = ("chip", "core")
    return jax.shard_map(
        per_device,
        mesh=split,
        in_specs=(
            P(every),
            P(every, None),
            P(gx, "gy", None, None, None),
            P(gx, "gy", None, None),
            P(gx, "gy", None),
        ),
        out_specs=(P(), P(gx, "gy", None)),
        check_vma=False,
    )
```

```python
import functools
import math

import jax
import jax.numpy as jnp
from jax import lax
from jax.experimental import pallas as pl
from jax.experimental.pallas import tpu as pltpu
from jax.sharding import Mesh
from jax.sharding import PartitionSpec as P


HOT = 2048
OWN_ROWS = 2048
LANES = 128
SUB = 8
SCALES = SUB // 2
STEPS = 128.0
TOP = 32600.0
TINY = 2.0**-100
ROOM = pltpu.CompilerParams(vmem_limit_bytes=20 * 2**20)


def in_hbm(array):
    return pltpu.with_memory_space_constraint(array, pltpu.HBM)


def masked_halves(keep, data_ref, rhs_ref, base, width):
    flags = keep.T
    for j in range(keep.shape[0]):
        rows = pl.ds(base + j * LANES, LANES)
        column = jnp.broadcast_to(flags[:, j : j + 1], (LANES, width)).astype(jnp.bfloat16)
        data = data_ref[pl.ds(j * LANES, LANES), :]
        kept = data * column
        rhs_ref[rows, :width] = kept
        rhs_ref[rows, width:] = data - kept


def onehot_block(row, start, size):
    places = (lax.broadcasted_iota(jnp.int32, (size, LANES), 0) + start).astype(jnp.int16)
    one, zero = jnp.ones((), jnp.bfloat16), jnp.zeros((), jnp.bfloat16)
    parts = [jnp.where(places == row[j : j + 1, :], one, zero) for j in range(row.shape[0])]
    return jnp.concatenate(parts, axis=1)


def hot_kernel(ids_ref, data_ref, mine_ref, send_ref, rhs_ref, *, block, step):
    half, width = mine_ref.shape
    core = lax.axis_index("core")
    lines = step // LANES
    for first in range(0, data_ref.shape[0], step):
        ids = ids_ref[pl.ds(first // LANES, lines), :]
        high = (ids >= half).astype(jnp.int32)
        masked_halves((high == core).astype(jnp.float32), data_ref.at[pl.ds(first, step)], rhs_ref, 0, width)
        row = (ids - high * half).astype(jnp.int16)
        rhs = rhs_ref[...]
        for start in range(0, half, block):
            part = jnp.dot(onehot_block(row, start, block), rhs, preferred_element_type=jnp.float32)
            rows = pl.ds(start, block)
            if first == 0:
                mine_ref[rows, :] = part[:, :width]
                send_ref[rows, :] = part[:, width:]
            else:
                mine_ref[rows, :] += part[:, :width]
                send_ref[rows, :] += part[:, width:]


def hot_sums(ids, data, table):
    lookups, width = data.shape
    half = table // 2
    step = math.gcd(lookups, 4096)
    whole = pl.BlockSpec(memory_space=pltpu.VMEM)
    return pl.pallas_call(
        functools.partial(hot_kernel, block=math.gcd(half, 256), step=step),
        in_specs=[whole, whole],
        out_specs=[whole, whole],
        out_shape=[jax.ShapeDtypeStruct((half, width), jnp.float32)] * 2,
        scratch_shapes=[pltpu.VMEM((step, 2 * width), jnp.bfloat16)],
        cost_estimate=pl.CostEstimate(flops=2 * lookups * table * width, bytes_accessed=2 * lookups * width, transcendentals=0),
        compiler_params=ROOM,
        name="hot_sums",
    )(ids.reshape(lookups // LANES, LANES), data)


def pick_kernel(blocks_hbm, *refs, steps):
    outs, sems = refs[:-1], refs[-1]
    owner, owners = lax.axis_index("gy"), blocks_hbm.shape[0]
    copies = [
        pltpu.make_async_copy(blocks_hbm.at[partner(owner, step, owners)[1]], out, sems.at[n])
        for n, (step, out) in enumerate(zip(steps, outs))
    ]
    for copy in copies:
        copy.start()
    for copy in copies:
        copy.wait()


def pick(blocks, steps):
    count = len(steps)
    return pl.pallas_call(
        functools.partial(pick_kernel, steps=steps),
        in_specs=[pl.BlockSpec(memory_space=pltpu.HBM)],
        out_specs=[pl.BlockSpec(memory_space=pltpu.VMEM)] * count,
        out_shape=[jax.ShapeDtypeStruct(blocks.shape[1:], blocks.dtype)] * count,
        scratch_shapes=[pltpu.SemaphoreType.DMA((count,))],
        cost_estimate=pl.CostEstimate(flops=5 * 10**9, bytes_accessed=count * blocks[0].size * 2, transcendentals=0),
        compiler_params=ROOM,
        name="pick",
    )(in_hbm(blocks))


def encode(values):
    rows, width = values.shape
    groups = values.reshape(rows // SUB, SUB, width)
    most = jnp.max(jnp.abs(groups), axis=0)
    most = jnp.maximum(jnp.maximum(most[:SCALES], most[SCALES:]), TINY)
    code = jnp.ceil(jnp.log2(most) * STEPS) + 1.0
    scale = jnp.exp2(code * (-1.0 / STEPS)) * TOP
    codes = jnp.round(groups * jnp.concatenate([scale, scale], axis=0)[None])
    return codes.reshape(rows, width), code


def decode(codes, code):
    rows, width = codes.shape
    scale = jnp.exp2(code * (1.0 / STEPS)) * (1.0 / TOP)
    scale = jnp.concatenate([scale, scale], axis=0)
    return (codes.reshape(rows // SUB, SUB, width) * scale[None]).reshape(rows, width)


def narrow(values):
    return values.astype(jnp.int32).astype(jnp.int16)


def widen(values):
    return values.astype(jnp.int32).astype(jnp.float32)


def tail_rows(lines):
    return -(-(SCALES + lines) // SUB) * SUB


def pack_kernel(mine_ref, got_ref, slots_ref, out_ref):
    owners, lines, _ = slots_ref.shape
    tail = tail_rows(lines)
    peers, rows, _ = out_ref.shape
    rows -= tail
    spare = tail - SCALES - lines
    for p in range(peers):
        here = pl.ds(p * rows, rows)
        codes, code = encode(mine_ref[here, :] + got_ref[here, :])
        out_ref[p, :rows, :] = narrow(codes)
        pieces = [code.astype(jnp.int32), slots_ref[p % owners]]
        if spare:
            pieces.append(jnp.zeros((spare, LANES), jnp.int32))
        out_ref[p, rows:, :] = jnp.concatenate(pieces, axis=0).astype(jnp.int16)


def pack(mine, got, slots, peers):
    half, width = mine.shape
    whole = pl.BlockSpec(memory_space=pltpu.VMEM)
    return pl.pallas_call(
        pack_kernel,
        in_specs=[whole, whole, whole],
        out_specs=whole,
        out_shape=jax.ShapeDtypeStruct((peers, half // peers + tail_rows(slots.shape[1]), width), jnp.int16),
        cost_estimate=pl.CostEstimate(flops=half * width * 8, bytes_accessed=half * width * 10, transcendentals=0),
        compiler_params=ROOM,
        name="pack",
    )(mine, got, slots)


def add_kernel(got_ref, out_ref, *, factor, tail):
    peers, rows, width = got_ref.shape
    rows -= tail
    total = jnp.zeros((rows, width), jnp.float32)
    for p in range(peers):
        ends = widen(got_ref[p, rows:, :])
        total += decode(widen(got_ref[p, :rows, :]), ends[:SCALES])
    codes, code = encode(total * factor)
    body, ends = narrow(codes), narrow(jnp.concatenate([code, code], axis=0))
    for p in range(peers):
        out_ref[p, :rows, :] = body
        out_ref[p, rows:, :] = ends


def add(got, factor, tail):
    peers, rows, width = got.shape
    whole = pl.BlockSpec(memory_space=pltpu.VMEM)
    return pl.pallas_call(
        functools.partial(add_kernel, factor=factor, tail=tail),
        in_specs=[whole],
        out_specs=whole,
        out_shape=jax.ShapeDtypeStruct((peers, rows - tail + SUB, width), jnp.int16),
        cost_estimate=pl.CostEstimate(flops=got.size * 8, bytes_accessed=got.size * 4, transcendentals=0),
        compiler_params=ROOM,
        name="add",
    )(got)


def unpack_kernel(mine_ref, other_ref, out_ref):
    peers, rows, _ = mine_ref.shape
    rows -= SUB
    core = lax.axis_index("core")
    for ref, side in ((mine_ref, core), (other_ref, 1 - core)):
        for p in range(peers):
            ends = widen(ref[p, rows:, :])
            start = pl.multiple_of(side * (peers * rows) + p * rows, SUB)
            out_ref[pl.ds(start, rows), :] = decode(widen(ref[p, :rows, :]), ends[:SCALES])


def unpack(mine, other, table):
    width = mine.shape[2]
    whole = pl.BlockSpec(memory_space=pltpu.VMEM)
    return pl.pallas_call(
        unpack_kernel,
        in_specs=[whole, whole],
        out_specs=whole,
        out_shape=jax.ShapeDtypeStruct((table, width), jnp.float32),
        cost_estimate=pl.CostEstimate(flops=table * width * 4, bytes_accessed=table * width * 6, transcendentals=0),
        compiler_params=ROOM,
        name="unpack",
    )(mine, other)


def partner(me, step, count):
    if count & (count - 1):
        return (me - step) % count, (me + step) % count
    return me ^ step, me ^ step


def cold_steps(owners):
    far, near = list(range(owners // 2, owners)), list(range(1, owners // 2))
    early = len(far) * 3 // 4
    return far[:early], far[early:] + near


def cold_kernel(got_ref, own_ref, *refs, block, at, lines):
    moved, (out_ref, rhs_ref, row_ref) = refs[:-3], refs[-3:]
    owners, capacity, width = own_ref.shape
    half = out_ref.shape[0] // 2
    chip, owner = lax.axis_index("chip"), lax.axis_index("gy")
    for step, ref in enumerate((own_ref.at[owner], *moved)):
        source, _ = partner(owner, step, owners)
        slots = got_ref[chip * owners + source, at:, :].astype(jnp.int32)[SCALES : SCALES + lines]
        high = (slots >= half).astype(jnp.int32)
        masked_halves((high == 0).astype(jnp.float32), ref, rhs_ref, step * capacity, width)
        row_ref[pl.ds(step * lines, lines), :] = slots - high * half
    row = row_ref[...].astype(jnp.int16)
    rhs = rhs_ref[...]
    for start in range(0, half, block):
        part = jnp.dot(onehot_block(row, start, block), rhs, preferred_element_type=jnp.float32)
        out_ref[pl.ds(start, block), :] = part[:, :width]
        out_ref[pl.ds(half + start, block), :] = part[:, width:]


def cold_sums(got, own, moved, table):
    owners, capacity, width = own.shape
    lines = capacity // LANES
    whole = pl.BlockSpec(memory_space=pltpu.VMEM)
    return pl.pallas_call(
        functools.partial(cold_kernel, block=math.gcd(table // 2, 256), at=got.shape[1] - tail_rows(lines), lines=lines),
        in_specs=[whole] * (2 + len(moved)),
        out_specs=whole,
        out_shape=jax.ShapeDtypeStruct((table, width), jnp.float32),
        scratch_shapes=[
            pltpu.VMEM((owners * capacity, 2 * width), jnp.bfloat16),
            pltpu.VMEM((owners * lines, LANES), jnp.int32),
        ],
        cost_estimate=pl.CostEstimate(flops=2 * owners * capacity * table * width, bytes_accessed=2 * owners * capacity * width, transcendentals=0),
        compiler_params=ROOM,
        name="cold_sums",
    )(got, own, *moved)


def per_device(hot_ids, hot_grads, cold_grads, cold_slots, cold_counts):
    groups, owners = lax.axis_size("chip"), lax.axis_size("gy")
    peers = groups * owners
    everyone = ("chip", "gy")
    swap = [(0, 1), (1, 0)]
    factor = (HOT / (hot_ids.shape[0] * peers * 2)) ** 0.5

    capacity, width = cold_grads.shape[3:]
    lines = capacity // LANES
    blocks = cold_grads.reshape(owners, capacity, width)
    moved = {}

    def move(steps):
        picked = pick(blocks, steps)
        for n, block in zip(steps, picked):
            moved[n] = lax.ppermute(block, "gy", [(i, partner(i, n, owners)[1]) for i in range(owners)])

    early, late = cold_steps(owners)
    move(early)
    mine, send = hot_sums(hot_ids, hot_grads, HOT)
    got = lax.ppermute(send, "core", swap)
    places = lax.broadcasted_iota(jnp.int32, (owners, capacity), 1)
    used = jnp.where(places < cold_counts.reshape(owners, 1), cold_slots.reshape(owners, capacity), -1)
    packed = pack(mine, got, used.reshape(owners, lines, LANES), peers)
    parts = lax.all_to_all(packed, everyone, split_axis=0, concat_axis=0, tiled=True)
    move(late)
    summed = add(parts, factor, tail_rows(lines))
    all_rows = lax.all_to_all(summed, everyone, split_axis=0, concat_axis=0, tiled=True)
    cold_grad = cold_sums(parts, blocks, [moved[n] for n in range(1, owners)], OWN_ROWS)
    others = lax.ppermute(all_rows, "core", swap)
    hot_grad = unpack(all_rows, others, HOT)
    return hot_grad, cold_grad.reshape(1, OWN_ROWS, width)


def solution(mesh):
    wide, owners = mesh.devices.shape
    split = Mesh(mesh.devices.reshape(wide // 2, 2, owners), ("chip", "core", "gy"))
    every = ("chip", "core", "gy")
    gx = ("chip", "core")
    return jax.shard_map(
        per_device,
        mesh=split,
        in_specs=(
            P(every),
            P(every, None),
            P(gx, "gy", None, None, None),
            P(gx, "gy", None, None),
            P(gx, "gy", None),
        ),
        out_specs=(P(), P(gx, "gy", None)),
        check_vma=False,
    )
```

```python
import functools
import math

import jax
import jax.numpy as jnp
from jax import lax
from jax.experimental import pallas as pl
from jax.experimental.pallas import tpu as pltpu
from jax.sharding import Mesh
from jax.sharding import PartitionSpec as P


HOT = 2048
OWN_ROWS = 2048
LANES = 128
SUB = 8
SCALES = SUB // 2
STEPS = 128.0
TOP = 32600.0
TINY = 2.0**-100
ROOM = pltpu.CompilerParams(vmem_limit_bytes=20 * 2**20)


def in_hbm(array):
    return pltpu.with_memory_space_constraint(array, pltpu.HBM)


def masked_halves(keep, data_ref, rhs_ref, base, width):
    flags = keep.T
    for j in range(keep.shape[0]):
        rows = pl.ds(base + j * LANES, LANES)
        column = jnp.broadcast_to(flags[:, j : j + 1], (LANES, width)).astype(jnp.bfloat16)
        data = data_ref[pl.ds(j * LANES, LANES), :]
        kept = data * column
        rhs_ref[rows, :width] = kept
        rhs_ref[rows, width:] = data - kept


def onehot_block(row, start, size):
    places = (lax.broadcasted_iota(jnp.int32, (size, LANES), 0) + start).astype(jnp.int16)
    one, zero = jnp.ones((), jnp.bfloat16), jnp.zeros((), jnp.bfloat16)
    parts = [jnp.where(places == row[j : j + 1, :], one, zero) for j in range(row.shape[0])]
    return jnp.concatenate(parts, axis=1)


def hot_kernel(ids_ref, data_ref, mine_ref, send_ref, rhs_ref, *, block, step):
    half, width = mine_ref.shape
    core = lax.axis_index("core")
    lines = step // LANES
    for first in range(0, data_ref.shape[0], step):
        ids = ids_ref[pl.ds(first // LANES, lines), :]
        high = (ids >= half).astype(jnp.int32)
        masked_halves((high == core).astype(jnp.float32), data_ref.at[pl.ds(first, step)], rhs_ref, 0, width)
        row = (ids - high * half).astype(jnp.int16)
        rhs = rhs_ref[...]
        for start in range(0, half, block):
            part = jnp.dot(onehot_block(row, start, block), rhs, preferred_element_type=jnp.float32)
            rows = pl.ds(start, block)
            if first == 0:
                mine_ref[rows, :] = part[:, :width]
                send_ref[rows, :] = part[:, width:]
            else:
                mine_ref[rows, :] += part[:, :width]
                send_ref[rows, :] += part[:, width:]


def hot_sums(ids, data, table):
    lookups, width = data.shape
    half = table // 2
    step = math.gcd(lookups, 4096)
    whole = pl.BlockSpec(memory_space=pltpu.VMEM)
    return pl.pallas_call(
        functools.partial(hot_kernel, block=math.gcd(half, 256), step=step),
        in_specs=[whole, whole],
        out_specs=[whole, whole],
        out_shape=[jax.ShapeDtypeStruct((half, width), jnp.float32)] * 2,
        scratch_shapes=[pltpu.VMEM((step, 2 * width), jnp.bfloat16)],
        cost_estimate=pl.CostEstimate(flops=2 * lookups * table * width, bytes_accessed=2 * lookups * width, transcendentals=0),
        compiler_params=ROOM,
        name="hot_sums",
    )(ids.reshape(lookups // LANES, LANES), data)


def pick_kernel(blocks_hbm, *refs, steps):
    outs, sems = refs[:-1], refs[-1]
    owner, owners = lax.axis_index("gy"), blocks_hbm.shape[0]
    copies = [
        pltpu.make_async_copy(blocks_hbm.at[partner(owner, step, owners)[1]], out, sems.at[n])
        for n, (step, out) in enumerate(zip(steps, outs))
    ]
    for copy in copies:
        copy.start()
    for copy in copies:
        copy.wait()


def pick(blocks, steps):
    count = len(steps)
    return pl.pallas_call(
        functools.partial(pick_kernel, steps=steps),
        in_specs=[pl.BlockSpec(memory_space=pltpu.HBM)],
        out_specs=[pl.BlockSpec(memory_space=pltpu.VMEM)] * count,
        out_shape=[jax.ShapeDtypeStruct(blocks.shape[1:], blocks.dtype)] * count,
        scratch_shapes=[pltpu.SemaphoreType.DMA((count,))],
        cost_estimate=pl.CostEstimate(flops=5 * 10**9, bytes_accessed=count * blocks[0].size * 2, transcendentals=0),
        compiler_params=ROOM,
        name="pick",
    )(in_hbm(blocks))


def encode(values):
    rows, width = values.shape
    groups = values.reshape(rows // SUB, SUB, width)
    most = jnp.max(jnp.abs(groups), axis=0)
    most = jnp.maximum(jnp.maximum(most[:SCALES], most[SCALES:]), TINY)
    code = jnp.ceil(jnp.log2(most) * STEPS) + 1.0
    scale = jnp.exp2(code * (-1.0 / STEPS)) * TOP
    codes = jnp.round(groups * jnp.concatenate([scale, scale], axis=0)[None])
    return codes.reshape(rows, width), code


def decode(codes, code):
    rows, width = codes.shape
    scale = jnp.exp2(code * (1.0 / STEPS)) * (1.0 / TOP)
    scale = jnp.concatenate([scale, scale], axis=0)
    return (codes.reshape(rows // SUB, SUB, width) * scale[None]).reshape(rows, width)


def narrow(values):
    return values.astype(jnp.int32).astype(jnp.int16)


def widen(values):
    return values.astype(jnp.int32).astype(jnp.float32)


def tail_rows(lines):
    return -(-(SCALES + lines) // SUB) * SUB


def pack_kernel(mine_ref, got_ref, own_ref, *out_refs):
    owners, rows, _ = out_refs[0].shape
    rows -= SUB
    groups = len(out_refs) + 1
    chip = lax.axis_index("chip")
    for step, out_ref in enumerate(out_refs, 1):
        base = partner(chip, step, groups)[1] * (owners * rows)
        for p in range(owners):
            here = pl.ds(pl.multiple_of(base + p * rows, SUB), rows)
            codes, code = encode(mine_ref[here, :] + got_ref[here, :])
            out_ref[p, :rows, :] = narrow(codes)
            out_ref[p, rows:, :] = narrow(jnp.concatenate([code, code], axis=0))
    here = pl.ds(pl.multiple_of(chip * (owners * rows), SUB), owners * rows)
    own_ref[...] = mine_ref[here, :] + got_ref[here, :]


def pack(mine, got, groups, owners):
    half, width = mine.shape
    rows = half // (groups * owners)
    whole = pl.BlockSpec(memory_space=pltpu.VMEM)
    own, *coded = pl.pallas_call(
        pack_kernel,
        in_specs=[whole, whole],
        out_specs=[whole] * groups,
        out_shape=[jax.ShapeDtypeStruct((owners * rows, width), jnp.float32)]
        + [jax.ShapeDtypeStruct((owners, rows + SUB, width), jnp.int16)] * (groups - 1),
        cost_estimate=pl.CostEstimate(flops=half * width * 8, bytes_accessed=half * width * 10, transcendentals=0),
        compiler_params=ROOM,
        name="pack",
    )(mine, got)
    return own, coded


def join_kernel(own_ref, slots_ref, *refs):
    got_refs, out_ref = refs[:-1], refs[-1]
    owners, lines, _ = slots_ref.shape
    tail = tail_rows(lines)
    rows = out_ref.shape[1] - tail
    spare = tail - SCALES - lines
    for p in range(owners):
        total = own_ref[p * rows : (p + 1) * rows, :]
        for ref in got_refs:
            ends = widen(ref[p, rows:, :])
            total += decode(widen(ref[p, :rows, :]), ends[:SCALES])
        codes, code = encode(total)
        out_ref[p, :rows, :] = narrow(codes)
        pieces = [code.astype(jnp.int32), slots_ref[p]]
        if spare:
            pieces.append(jnp.zeros((spare, LANES), jnp.int32))
        out_ref[p, rows:, :] = jnp.concatenate(pieces, axis=0).astype(jnp.int16)


def join(own, slots, got):
    owners, lines, _ = slots.shape
    total, width = own.shape
    whole = pl.BlockSpec(memory_space=pltpu.VMEM)
    return pl.pallas_call(
        join_kernel,
        in_specs=[whole] * (2 + len(got)),
        out_specs=whole,
        out_shape=jax.ShapeDtypeStruct((owners, total // owners + tail_rows(lines), width), jnp.int16),
        cost_estimate=pl.CostEstimate(flops=total * width * 8, bytes_accessed=total * width * 10, transcendentals=0),
        compiler_params=ROOM,
        name="join",
    )(own, slots, *got)


def add_kernel(got_ref, out_ref, *, factor, tail):
    peers, rows, width = got_ref.shape
    rows -= tail
    total = jnp.zeros((rows, width), jnp.float32)
    for p in range(peers):
        ends = widen(got_ref[p, rows:, :])
        total += decode(widen(got_ref[p, :rows, :]), ends[:SCALES])
    codes, code = encode(total * factor)
    body, ends = narrow(codes), narrow(jnp.concatenate([code, code], axis=0))
    for p in range(out_ref.shape[0]):
        out_ref[p, :rows, :] = body
        out_ref[p, rows:, :] = ends


def add(got, factor, tail, copies):
    _, rows, width = got.shape
    whole = pl.BlockSpec(memory_space=pltpu.VMEM)
    return pl.pallas_call(
        functools.partial(add_kernel, factor=factor, tail=tail),
        in_specs=[whole],
        out_specs=whole,
        out_shape=jax.ShapeDtypeStruct((copies, rows - tail + SUB, width), jnp.int16),
        cost_estimate=pl.CostEstimate(flops=got.size * 8, bytes_accessed=got.size * 4, transcendentals=0),
        compiler_params=ROOM,
        name="add",
    )(got)


def unpack_kernel(mine_ref, other_ref, out_ref):
    peers, rows, _ = mine_ref.shape
    rows -= SUB
    core = lax.axis_index("core")
    for ref, side in ((mine_ref, core), (other_ref, 1 - core)):
        for p in range(peers):
            ends = widen(ref[p, rows:, :])
            start = pl.multiple_of(side * (peers * rows) + p * rows, SUB)
            out_ref[pl.ds(start, rows), :] = decode(widen(ref[p, :rows, :]), ends[:SCALES])


def unpack(mine, other, table):
    width = mine.shape[2]
    whole = pl.BlockSpec(memory_space=pltpu.VMEM)
    return pl.pallas_call(
        unpack_kernel,
        in_specs=[whole, whole],
        out_specs=whole,
        out_shape=jax.ShapeDtypeStruct((table, width), jnp.float32),
        cost_estimate=pl.CostEstimate(flops=table * width * 4, bytes_accessed=table * width * 6, transcendentals=0),
        compiler_params=ROOM,
        name="unpack",
    )(mine, other)


def partner(me, step, count):
    if count & (count - 1):
        return (me - step) % count, (me + step) % count
    return me ^ step, me ^ step


def cold_steps(owners):
    far, near = list(range(owners // 2, owners)), list(range(1, owners // 2))
    a, b, c, n = len(far) // 4, len(far) // 2, len(far) * 3 // 4, len(near) * 2 // 3
    return far[:a], far[a:b], far[b:c] + near[:n], far[c:] + near[n:]


def cold_kernel(got_ref, own_ref, *refs, block, at, lines):
    moved, (out_ref, rhs_ref, row_ref) = refs[:-3], refs[-3:]
    owners, capacity, width = own_ref.shape
    half = out_ref.shape[0] // 2
    owner = lax.axis_index("gy")
    for step, ref in enumerate((own_ref.at[owner], *moved)):
        source, _ = partner(owner, step, owners)
        slots = got_ref[source, at:, :].astype(jnp.int32)[SCALES : SCALES + lines]
        high = (slots >= half).astype(jnp.int32)
        masked_halves((high == 0).astype(jnp.float32), ref, rhs_ref, step * capacity, width)
        row_ref[pl.ds(step * lines, lines), :] = slots - high * half
    row = row_ref[...].astype(jnp.int16)
    rhs = rhs_ref[...]
    for start in range(0, half, block):
        part = jnp.dot(onehot_block(row, start, block), rhs, preferred_element_type=jnp.float32)
        out_ref[pl.ds(start, block), :] = part[:, :width]
        out_ref[pl.ds(half + start, block), :] = part[:, width:]


def cold_sums(got, own, moved, table):
    owners, capacity, width = own.shape
    lines = capacity // LANES
    whole = pl.BlockSpec(memory_space=pltpu.VMEM)
    return pl.pallas_call(
        functools.partial(cold_kernel, block=math.gcd(table // 2, 256), at=got.shape[1] - tail_rows(lines), lines=lines),
        in_specs=[whole] * (2 + len(moved)),
        out_specs=whole,
        out_shape=jax.ShapeDtypeStruct((table, width), jnp.float32),
        scratch_shapes=[
            pltpu.VMEM((owners * capacity, 2 * width), jnp.bfloat16),
            pltpu.VMEM((owners * lines, LANES), jnp.int32),
        ],
        cost_estimate=pl.CostEstimate(flops=2 * owners * capacity * table * width, bytes_accessed=2 * owners * capacity * width, transcendentals=0),
        compiler_params=ROOM,
        name="cold_sums",
    )(got, own, *moved)


def per_device(hot_ids, hot_grads, cold_grads, cold_slots, cold_counts):
    groups, owners = lax.axis_size("chip"), lax.axis_size("gy")
    peers = groups * owners
    everyone = ("chip", "gy")
    swap = [(0, 1), (1, 0)]
    factor = (HOT / (hot_ids.shape[0] * peers * 2)) ** 0.5

    capacity, width = cold_grads.shape[3:]
    lines = capacity // LANES
    blocks = cold_grads.reshape(owners, capacity, width)
    moved = {}

    def take(steps):
        if not steps:
            return {}
        return dict(zip(steps, pick(blocks, steps)))

    def move(picked, steps):
        for n in steps:
            moved[n] = lax.ppermute(picked[n], "gy", [(i, partner(i, n, owners)[1]) for i in range(owners)])

    early, middle, third, late = cold_steps(owners)
    picked = take(early + middle)
    move(picked, early)
    mine, send = hot_sums(hot_ids, hot_grads, HOT)
    got = lax.ppermute(send, "core", swap)
    move(picked, middle)
    places = lax.broadcasted_iota(jnp.int32, (owners, capacity), 1)
    used = jnp.where(places < cold_counts.reshape(owners, 1), cold_slots.reshape(owners, capacity), -1)
    own, coded = pack(mine, got, groups, owners)
    crossed = []
    for n, block in enumerate(coded, 1):
        crossed.append(lax.ppermute(block, "chip", [(i, partner(i, n, groups)[1]) for i in range(groups)]))
    move(take(third), third)
    joined = join(own, used.reshape(owners, lines, LANES), crossed)
    parts = lax.all_to_all(joined, "gy", split_axis=0, concat_axis=0, tiled=True)
    move(take(late), late)
    summed = add(parts, factor, tail_rows(lines), peers)
    all_rows = lax.all_to_all(summed, everyone, split_axis=0, concat_axis=0, tiled=True)
    cold_grad = cold_sums(parts, blocks, [moved[n] for n in range(1, owners)], OWN_ROWS)
    others = lax.ppermute(all_rows, "core", swap)
    hot_grad = unpack(all_rows, others, HOT)
    return hot_grad, cold_grad.reshape(1, OWN_ROWS, width)


def solution(mesh):
    wide, owners = mesh.devices.shape
    split = Mesh(mesh.devices.reshape(wide // 2, 2, owners), ("chip", "core", "gy"))
    every = ("chip", "core", "gy")
    gx = ("chip", "core")
    return jax.shard_map(
        per_device,
        mesh=split,
        in_specs=(
            P(every),
            P(every, None),
            P(gx, "gy", None, None, None),
            P(gx, "gy", None, None),
            P(gx, "gy", None),
        ),
        out_specs=(P(), P(gx, "gy", None)),
        check_vma=False,
    )
```

```python
import functools
import math

import jax
import jax.numpy as jnp
from jax import lax
from jax.experimental import pallas as pl
from jax.experimental.pallas import tpu as pltpu
from jax.sharding import Mesh
from jax.sharding import PartitionSpec as P


HOT = 2048
OWN_ROWS = 2048
LANES = 128
SUB = 8
SCALES = SUB // 2
STEPS = 128.0
TOP = 32600.0
TINY = 2.0**-100
ROOM = pltpu.CompilerParams(vmem_limit_bytes=20 * 2**20)


def in_hbm(array):
    return pltpu.with_memory_space_constraint(array, pltpu.HBM)


def masked_halves(keep, data_refs, rhs_ref, base, width):
    flags = keep.T
    for j in range(keep.shape[0]):
        rows = pl.ds(base + j * LANES, LANES)
        column = jnp.broadcast_to(flags[:, j : j + 1], (LANES, width)).astype(jnp.bfloat16)
        data = sum(ref[pl.ds(j * LANES, LANES), :] for ref in data_refs)
        kept = data * column
        rhs_ref[rows, :width] = kept
        rhs_ref[rows, width:] = data - kept


def onehot_block(row, start, size):
    places = (lax.broadcasted_iota(jnp.int32, (size, LANES), 0) + start).astype(jnp.int16)
    one, zero = jnp.ones((), jnp.bfloat16), jnp.zeros((), jnp.bfloat16)
    parts = [jnp.where(places == row[j : j + 1, :], one, zero) for j in range(row.shape[0])]
    return jnp.concatenate(parts, axis=1)


def hot_kernel(ids_ref, data_ref, mine_ref, send_ref, rhs_ref, *, block, step):
    half, width = mine_ref.shape
    core = lax.axis_index("core")
    lines = step // LANES
    for first in range(0, data_ref.shape[0], step):
        ids = ids_ref[pl.ds(first // LANES, lines), :]
        high = (ids >= half).astype(jnp.int32)
        masked_halves((high == core).astype(jnp.float32), [data_ref.at[pl.ds(first, step)]], rhs_ref, 0, width)
        row = (ids - high * half).astype(jnp.int16)
        rhs = rhs_ref[...]
        for start in range(0, half, block):
            part = jnp.dot(onehot_block(row, start, block), rhs, preferred_element_type=jnp.float32)
            rows = pl.ds(start, block)
            if first == 0:
                mine_ref[rows, :] = part[:, :width]
                send_ref[rows, :] = part[:, width:]
            else:
                mine_ref[rows, :] += part[:, :width]
                send_ref[rows, :] += part[:, width:]


def hot_sums(ids, data, table):
    lookups, width = data.shape
    half = table // 2
    step = math.gcd(lookups, 4096)
    whole = pl.BlockSpec(memory_space=pltpu.VMEM)
    return pl.pallas_call(
        functools.partial(hot_kernel, block=math.gcd(half, 256), step=step),
        in_specs=[whole, whole],
        out_specs=[whole, whole],
        out_shape=[jax.ShapeDtypeStruct((half, width), jnp.float32)] * 2,
        scratch_shapes=[pltpu.VMEM((step, 2 * width), jnp.bfloat16)],
        cost_estimate=pl.CostEstimate(flops=2 * lookups * table * width, bytes_accessed=2 * lookups * width, transcendentals=0),
        compiler_params=ROOM,
        name="hot_sums",
    )(ids.reshape(lookups // LANES, LANES), data)


def pick_kernel(blocks_hbm, *refs, steps):
    outs, sems = refs[:-1], refs[-1]
    owner, owners = lax.axis_index("gy"), blocks_hbm.shape[0]
    copies = [
        pltpu.make_async_copy(blocks_hbm.at[partner(owner, step, owners)[1]], out, sems.at[n])
        for n, (step, out) in enumerate(zip(steps, outs))
    ]
    for copy in copies:
        copy.start()
    for copy in copies:
        copy.wait()


def pick(blocks, steps):
    count = len(steps)
    return pl.pallas_call(
        functools.partial(pick_kernel, steps=steps),
        in_specs=[pl.BlockSpec(memory_space=pltpu.HBM)],
        out_specs=[pl.BlockSpec(memory_space=pltpu.VMEM)] * count,
        out_shape=[jax.ShapeDtypeStruct(blocks.shape[1:], blocks.dtype)] * count,
        scratch_shapes=[pltpu.SemaphoreType.DMA((count,))],
        cost_estimate=pl.CostEstimate(flops=5 * 10**9, bytes_accessed=count * blocks[0].size * 2, transcendentals=0),
        compiler_params=ROOM,
        name="pick",
    )(in_hbm(blocks))


def encode(values):
    rows, width = values.shape
    groups = values.reshape(rows // SUB, SUB, width)
    most = jnp.max(jnp.abs(groups), axis=0)
    most = jnp.maximum(jnp.maximum(most[:SCALES], most[SCALES:]), TINY)
    code = jnp.ceil(jnp.log2(most) * STEPS) + 1.0
    scale = jnp.exp2(code * (-1.0 / STEPS)) * TOP
    codes = jnp.round(groups * jnp.concatenate([scale, scale], axis=0)[None])
    return codes.reshape(rows, width), code


def decode(codes, code):
    rows, width = codes.shape
    scale = jnp.exp2(code * (1.0 / STEPS)) * (1.0 / TOP)
    scale = jnp.concatenate([scale, scale], axis=0)
    return (codes.reshape(rows // SUB, SUB, width) * scale[None]).reshape(rows, width)


def narrow(values):
    return values.astype(jnp.int32).astype(jnp.int16)


def widen(values):
    return values.astype(jnp.int32).astype(jnp.float32)


def tail_rows(lines):
    return -(-(SCALES + lines) // SUB) * SUB


def pack_kernel(mine_ref, got_ref, own_ref, *out_refs):
    owners, rows, _ = out_refs[0].shape
    rows -= SUB
    groups = len(out_refs) + 1
    chip = lax.axis_index("chip")
    for step, out_ref in enumerate(out_refs, 1):
        base = partner(chip, step, groups)[1] * (owners * rows)
        for p in range(owners):
            here = pl.ds(pl.multiple_of(base + p * rows, SUB), rows)
            codes, code = encode(mine_ref[here, :] + got_ref[here, :])
            out_ref[p, :rows, :] = narrow(codes)
            out_ref[p, rows:, :] = narrow(jnp.concatenate([code, code], axis=0))
    here = pl.ds(pl.multiple_of(chip * (owners * rows), SUB), owners * rows)
    own_ref[...] = mine_ref[here, :] + got_ref[here, :]


def pack(mine, got, groups, owners):
    half, width = mine.shape
    rows = half // (groups * owners)
    whole = pl.BlockSpec(memory_space=pltpu.VMEM)
    own, *coded = pl.pallas_call(
        pack_kernel,
        in_specs=[whole, whole],
        out_specs=[whole] * groups,
        out_shape=[jax.ShapeDtypeStruct((owners * rows, width), jnp.float32)]
        + [jax.ShapeDtypeStruct((owners, rows + SUB, width), jnp.int16)] * (groups - 1),
        cost_estimate=pl.CostEstimate(flops=half * width * 8, bytes_accessed=half * width * 10, transcendentals=0),
        compiler_params=ROOM,
        name="pack",
    )(mine, got)
    return own, coded


def join_kernel(own_ref, slots_ref, *refs):
    got_refs, out_ref = refs[:-1], refs[-1]
    owners, lines, _ = slots_ref.shape
    tail = tail_rows(lines)
    rows = out_ref.shape[1] - tail
    spare = tail - SCALES - lines
    for p in range(owners):
        total = own_ref[p * rows : (p + 1) * rows, :]
        for ref in got_refs:
            ends = widen(ref[p, rows:, :])
            total += decode(widen(ref[p, :rows, :]), ends[:SCALES])
        codes, code = encode(total)
        out_ref[p, :rows, :] = narrow(codes)
        pieces = [code.astype(jnp.int32), slots_ref[p]]
        if spare:
            pieces.append(jnp.zeros((spare, LANES), jnp.int32))
        out_ref[p, rows:, :] = jnp.concatenate(pieces, axis=0).astype(jnp.int16)


def join(own, slots, got):
    owners, lines, _ = slots.shape
    total, width = own.shape
    whole = pl.BlockSpec(memory_space=pltpu.VMEM)
    return pl.pallas_call(
        join_kernel,
        in_specs=[whole] * (2 + len(got)),
        out_specs=whole,
        out_shape=jax.ShapeDtypeStruct((owners, total // owners + tail_rows(lines), width), jnp.int16),
        cost_estimate=pl.CostEstimate(flops=total * width * 8, bytes_accessed=total * width * 10, transcendentals=0),
        compiler_params=ROOM,
        name="join",
    )(own, slots, *got)


def add_kernel(got_ref, out_ref, *, factor, tail):
    peers, rows, width = got_ref.shape
    rows -= tail
    total = jnp.zeros((rows, width), jnp.float32)
    for p in range(peers):
        ends = widen(got_ref[p, rows:, :])
        total += decode(widen(got_ref[p, :rows, :]), ends[:SCALES])
    codes, code = encode(total * factor)
    body, ends = narrow(codes), narrow(jnp.concatenate([code, code], axis=0))
    for p in range(out_ref.shape[0]):
        out_ref[p, :rows, :] = body
        out_ref[p, rows:, :] = ends


def add(got, factor, tail, copies):
    _, rows, width = got.shape
    whole = pl.BlockSpec(memory_space=pltpu.VMEM)
    return pl.pallas_call(
        functools.partial(add_kernel, factor=factor, tail=tail),
        in_specs=[whole],
        out_specs=whole,
        out_shape=jax.ShapeDtypeStruct((copies, rows - tail + SUB, width), jnp.int16),
        cost_estimate=pl.CostEstimate(flops=got.size * 8, bytes_accessed=got.size * 4, transcendentals=0),
        compiler_params=ROOM,
        name="add",
    )(got)


def unpack_kernel(mine_ref, other_ref, out_ref):
    peers, rows, _ = mine_ref.shape
    rows -= SUB
    core = lax.axis_index("core")
    for ref, side in ((mine_ref, core), (other_ref, 1 - core)):
        for p in range(peers):
            ends = widen(ref[p, rows:, :])
            start = pl.multiple_of(side * (peers * rows) + p * rows, SUB)
            out_ref[pl.ds(start, rows), :] = decode(widen(ref[p, :rows, :]), ends[:SCALES])


def unpack(mine, other, table):
    width = mine.shape[2]
    whole = pl.BlockSpec(memory_space=pltpu.VMEM)
    return pl.pallas_call(
        unpack_kernel,
        in_specs=[whole, whole],
        out_specs=whole,
        out_shape=jax.ShapeDtypeStruct((table, width), jnp.float32),
        cost_estimate=pl.CostEstimate(flops=table * width * 4, bytes_accessed=table * width * 6, transcendentals=0),
        compiler_params=ROOM,
        name="unpack",
    )(mine, other)


def partner(me, step, count):
    if count & (count - 1):
        return (me - step) % count, (me + step) % count
    return me ^ step, me ^ step


def cold_lots(owners):
    far, near = list(range(owners // 2, owners)), list(range(1, owners // 2))
    a, b, c = len(far) // 4, len(far) // 2, len(far) * 3 // 4
    return far[:a], far[a:b], far[b:c], near + far[c:]


def cold_kernel(got_ref, own_ref, *refs, block, at, lines, steps):
    moved, (out_ref, rhs_ref, row_ref) = refs[:-3], refs[-3:]
    owners, capacity, width = own_ref.shape
    half = out_ref.shape[0] // 2
    owner = lax.axis_index("gy")
    for step in range(owners):
        blocks = [ref for ref, n in zip(moved, steps) if n == step] or [own_ref.at[owner]]
        source, _ = partner(owner, step, owners)
        slots = got_ref[source, at:, :].astype(jnp.int32)[SCALES : SCALES + lines]
        high = (slots >= half).astype(jnp.int32)
        masked_halves((high == 0).astype(jnp.float32), blocks, rhs_ref, step * capacity, width)
        row_ref[pl.ds(step * lines, lines), :] = slots - high * half
    row = row_ref[...].astype(jnp.int16)
    rhs = rhs_ref[...]
    for start in range(0, half, block):
        part = jnp.dot(onehot_block(row, start, block), rhs, preferred_element_type=jnp.float32)
        out_ref[pl.ds(start, block), :] = part[:, :width]
        out_ref[pl.ds(half + start, block), :] = part[:, width:]


def cold_sums(got, own, moved, steps, table):
    owners, capacity, width = own.shape
    lines = capacity // LANES
    whole = pl.BlockSpec(memory_space=pltpu.VMEM)
    return pl.pallas_call(
        functools.partial(
            cold_kernel, block=math.gcd(table // 2, 256), at=got.shape[1] - tail_rows(lines), lines=lines, steps=steps
        ),
        in_specs=[whole] * (2 + len(moved)),
        out_specs=whole,
        out_shape=jax.ShapeDtypeStruct((table, width), jnp.float32),
        scratch_shapes=[
            pltpu.VMEM((owners * capacity, 2 * width), jnp.bfloat16),
            pltpu.VMEM((owners * lines, LANES), jnp.int32),
        ],
        cost_estimate=pl.CostEstimate(flops=2 * owners * capacity * table * width, bytes_accessed=2 * owners * capacity * width, transcendentals=0),
        compiler_params=ROOM,
        name="cold_sums",
    )(got, own, *moved)


def per_device(hot_ids, hot_grads, cold_grads, cold_slots, cold_counts):
    groups, owners = lax.axis_size("chip"), lax.axis_size("gy")
    peers = groups * owners
    everyone = ("chip", "gy")
    swap = [(0, 1), (1, 0)]
    factor = (HOT / (hot_ids.shape[0] * peers * 2)) ** 0.5

    capacity, width = cold_grads.shape[3:]
    lines = capacity // LANES
    blocks = cold_grads.reshape(owners, capacity, width)
    picked, moved = {}, []

    def take(*lots):
        steps = sorted({n for lot in lots for n in lot} - set(picked))
        if steps:
            picked.update(zip(steps, pick(blocks, steps)))

    def move(lot):
        for n in lot:
            pairs = [(i, partner(i, n, owners)[1]) for i in range(owners)]
            moved.append((n, lax.ppermute(picked[n], "gy", pairs)))

    early, middle, third, late = cold_lots(owners)
    take(early, middle)
    move(early)
    mine, send = hot_sums(hot_ids, hot_grads, HOT)
    got = lax.ppermute(send, "core", swap)
    move(middle)
    places = lax.broadcasted_iota(jnp.int32, (owners, capacity), 1)
    used = jnp.where(places < cold_counts.reshape(owners, 1), cold_slots.reshape(owners, capacity), -1)
    own, coded = pack(mine, got, groups, owners)
    crossed = []
    for n, block in enumerate(coded, 1):
        crossed.append(lax.ppermute(block, "chip", [(i, partner(i, n, groups)[1]) for i in range(groups)]))
    take(third, late)
    move(third)
    joined = join(own, used.reshape(owners, lines, LANES), crossed)
    parts = lax.all_to_all(joined, "gy", split_axis=0, concat_axis=0, tiled=True)
    move(late)
    summed = add(parts, factor, tail_rows(lines), peers)
    all_rows = lax.all_to_all(summed, everyone, split_axis=0, concat_axis=0, tiled=True)
    cold_grad = cold_sums(parts, blocks, [block for _, block in moved], [n for n, _ in moved], OWN_ROWS)
    others = lax.ppermute(all_rows, "core", swap)
    hot_grad = unpack(all_rows, others, HOT)
    return hot_grad, cold_grad.reshape(1, OWN_ROWS, width)


def solution(mesh):
    wide, owners = mesh.devices.shape
    split = Mesh(mesh.devices.reshape(wide // 2, 2, owners), ("chip", "core", "gy"))
    every = ("chip", "core", "gy")
    gx = ("chip", "core")
    return jax.shard_map(
        per_device,
        mesh=split,
        in_specs=(
            P(every),
            P(every, None),
            P(gx, "gy", None, None, None),
            P(gx, "gy", None, None),
            P(gx, "gy", None),
        ),
        out_specs=(P(), P(gx, "gy", None)),
        check_vma=False,
    )
```

```python
import functools
import math

import jax
import jax.numpy as jnp
from jax import lax
from jax.experimental import pallas as pl
from jax.experimental.pallas import tpu as pltpu
from jax.sharding import Mesh
from jax.sharding import PartitionSpec as P


HOT = 2048
OWN_ROWS = 2048
LANES = 128
SUB = 8
SCALES = SUB // 2
STEPS = 128.0
TOP = 32600.0
TINY = 2.0**-100
ROOM = pltpu.CompilerParams(vmem_limit_bytes=20 * 2**20)


def in_hbm(array):
    return pltpu.with_memory_space_constraint(array, pltpu.HBM)


def masked_halves(keep, data_refs, rhs_ref, base, width):
    flags = keep.T
    for j in range(keep.shape[0]):
        rows = pl.ds(base + j * LANES, LANES)
        column = jnp.broadcast_to(flags[:, j : j + 1], (LANES, width)).astype(jnp.bfloat16)
        data = sum(ref[pl.ds(j * LANES, LANES), :] for ref in data_refs)
        kept = data * column
        rhs_ref[rows, :width] = kept
        rhs_ref[rows, width:] = data - kept


def onehot_block(row, start, size):
    places = (lax.broadcasted_iota(jnp.int32, (size, LANES), 0) + start).astype(jnp.int16)
    one, zero = jnp.ones((), jnp.bfloat16), jnp.zeros((), jnp.bfloat16)
    parts = [jnp.where(places == row[j : j + 1, :], one, zero) for j in range(row.shape[0])]
    return jnp.concatenate(parts, axis=1)


def hot_kernel(ids_ref, data_ref, mine_ref, send_ref, rhs_ref, *, block, step):
    half, width = mine_ref.shape
    core = lax.axis_index("core")
    lines = step // LANES
    for first in range(0, data_ref.shape[0], step):
        ids = ids_ref[pl.ds(first // LANES, lines), :]
        high = (ids >= half).astype(jnp.int32)
        masked_halves((high == core).astype(jnp.float32), [data_ref.at[pl.ds(first, step)]], rhs_ref, 0, width)
        row = (ids - high * half).astype(jnp.int16)
        rhs = rhs_ref[...]
        for start in range(0, half, block):
            part = jnp.dot(onehot_block(row, start, block), rhs, preferred_element_type=jnp.float32)
            rows = pl.ds(start, block)
            if first == 0:
                mine_ref[rows, :] = part[:, :width]
                send_ref[rows, :] = part[:, width:]
            else:
                mine_ref[rows, :] += part[:, :width]
                send_ref[rows, :] += part[:, width:]


def hot_sums(ids, data, table):
    lookups, width = data.shape
    half = table // 2
    step = math.gcd(lookups, 4096)
    whole = pl.BlockSpec(memory_space=pltpu.VMEM)
    return pl.pallas_call(
        functools.partial(hot_kernel, block=math.gcd(half, 256), step=step),
        in_specs=[whole, whole],
        out_specs=[whole, whole],
        out_shape=[jax.ShapeDtypeStruct((half, width), jnp.float32)] * 2,
        scratch_shapes=[pltpu.VMEM((step, 2 * width), jnp.bfloat16)],
        cost_estimate=pl.CostEstimate(flops=2 * lookups * table * width, bytes_accessed=2 * lookups * width, transcendentals=0),
        compiler_params=ROOM,
        name="hot_sums",
    )(ids.reshape(lookups // LANES, LANES), data)


def pick_kernel(blocks_hbm, *refs, steps):
    outs, sems = refs[:-1], refs[-1]
    owner, owners = lax.axis_index("gy"), blocks_hbm.shape[0]
    copies = [
        pltpu.make_async_copy(blocks_hbm.at[partner(owner, step, owners)[1]], out, sems.at[n])
        for n, (step, out) in enumerate(zip(steps, outs))
    ]
    for copy in copies:
        copy.start()
    for copy in copies:
        copy.wait()


def pick(blocks, steps):
    count = len(steps)
    return pl.pallas_call(
        functools.partial(pick_kernel, steps=steps),
        in_specs=[pl.BlockSpec(memory_space=pltpu.HBM)],
        out_specs=[pl.BlockSpec(memory_space=pltpu.VMEM)] * count,
        out_shape=[jax.ShapeDtypeStruct(blocks.shape[1:], blocks.dtype)] * count,
        scratch_shapes=[pltpu.SemaphoreType.DMA((count,))],
        cost_estimate=pl.CostEstimate(flops=5 * 10**9, bytes_accessed=count * blocks[0].size * 2, transcendentals=0),
        compiler_params=ROOM,
        name="pick",
    )(in_hbm(blocks))


def encode(values):
    rows, width = values.shape
    groups = values.reshape(rows // SUB, SUB, width)
    most = jnp.max(jnp.abs(groups), axis=0)
    most = jnp.maximum(jnp.maximum(most[:SCALES], most[SCALES:]), TINY)
    code = jnp.ceil(jnp.log2(most) * STEPS) + 1.0
    scale = jnp.exp2(code * (-1.0 / STEPS)) * TOP
    codes = jnp.round(groups * jnp.concatenate([scale, scale], axis=0)[None])
    return codes.reshape(rows, width), code


def decode(codes, code):
    rows, width = codes.shape
    scale = jnp.exp2(code * (1.0 / STEPS)) * (1.0 / TOP)
    scale = jnp.concatenate([scale, scale], axis=0)
    return (codes.reshape(rows // SUB, SUB, width) * scale[None]).reshape(rows, width)


def narrow(values):
    return values.astype(jnp.int32).astype(jnp.int16)


def widen(values):
    return values.astype(jnp.int32).astype(jnp.float32)


def tail_rows(lines):
    return -(-(SCALES + lines) // SUB) * SUB


def pack_kernel(mine_ref, got_ref, own_ref, *out_refs):
    owners, rows, _ = out_refs[0].shape
    rows -= SUB
    groups = len(out_refs) + 1
    chip = lax.axis_index("chip")
    for step, out_ref in enumerate(out_refs, 1):
        base = partner(chip, step, groups)[1] * (owners * rows)
        for p in range(owners):
            here = pl.ds(pl.multiple_of(base + p * rows, SUB), rows)
            codes, code = encode(mine_ref[here, :] + got_ref[here, :])
            out_ref[p, :rows, :] = narrow(codes)
            out_ref[p, rows:, :] = narrow(jnp.concatenate([code, code], axis=0))
    here = pl.ds(pl.multiple_of(chip * (owners * rows), SUB), owners * rows)
    own_ref[...] = mine_ref[here, :] + got_ref[here, :]


def pack(mine, got, groups, owners):
    half, width = mine.shape
    rows = half // (groups * owners)
    whole = pl.BlockSpec(memory_space=pltpu.VMEM)
    own, *coded = pl.pallas_call(
        pack_kernel,
        in_specs=[whole, whole],
        out_specs=[whole] * groups,
        out_shape=[jax.ShapeDtypeStruct((owners * rows, width), jnp.float32)]
        + [jax.ShapeDtypeStruct((owners, rows + SUB, width), jnp.int16)] * (groups - 1),
        cost_estimate=pl.CostEstimate(flops=half * width * 8, bytes_accessed=half * width * 10, transcendentals=0),
        compiler_params=ROOM,
        name="pack",
    )(mine, got)
    return own, coded


def join_kernel(own_ref, slots_ref, *refs):
    got_refs, out_ref = refs[:-1], refs[-1]
    owners, lines, _ = slots_ref.shape
    tail = tail_rows(lines)
    rows = out_ref.shape[1] - tail
    spare = tail - SCALES - lines
    for p in range(owners):
        total = own_ref[p * rows : (p + 1) * rows, :]
        for ref in got_refs:
            ends = widen(ref[p, rows:, :])
            total += decode(widen(ref[p, :rows, :]), ends[:SCALES])
        codes, code = encode(total)
        out_ref[p, :rows, :] = narrow(codes)
        pieces = [code.astype(jnp.int32), slots_ref[p]]
        if spare:
            pieces.append(jnp.zeros((spare, LANES), jnp.int32))
        out_ref[p, rows:, :] = jnp.concatenate(pieces, axis=0).astype(jnp.int16)


def join(own, slots, got):
    owners, lines, _ = slots.shape
    total, width = own.shape
    whole = pl.BlockSpec(memory_space=pltpu.VMEM)
    return pl.pallas_call(
        join_kernel,
        in_specs=[whole] * (2 + len(got)),
        out_specs=whole,
        out_shape=jax.ShapeDtypeStruct((owners, total // owners + tail_rows(lines), width), jnp.int16),
        cost_estimate=pl.CostEstimate(flops=total * width * 8, bytes_accessed=total * width * 10, transcendentals=0),
        compiler_params=ROOM,
        name="join",
    )(own, slots, *got)


def add_kernel(got_ref, out_ref, *, factor, tail):
    peers, rows, width = got_ref.shape
    rows -= tail
    total = jnp.zeros((rows, width), jnp.float32)
    for p in range(peers):
        ends = widen(got_ref[p, rows:, :])
        total += decode(widen(got_ref[p, :rows, :]), ends[:SCALES])
    codes, code = encode(total * factor)
    body, ends = narrow(codes), narrow(jnp.concatenate([code, code], axis=0))
    for p in range(out_ref.shape[0]):
        out_ref[p, :rows, :] = body
        out_ref[p, rows:, :] = ends


def add(got, factor, tail, copies):
    _, rows, width = got.shape
    whole = pl.BlockSpec(memory_space=pltpu.VMEM)
    return pl.pallas_call(
        functools.partial(add_kernel, factor=factor, tail=tail),
        in_specs=[whole],
        out_specs=whole,
        out_shape=jax.ShapeDtypeStruct((copies, rows - tail + SUB, width), jnp.int16),
        cost_estimate=pl.CostEstimate(flops=got.size * 8, bytes_accessed=got.size * 4, transcendentals=0),
        compiler_params=ROOM,
        name="add",
    )(got)


def unpack_kernel(codes_ref, *refs, flip):
    out_hbm, half_ref, sems = refs[-3:]
    peers, rows, _ = codes_ref.shape
    rows -= SUB
    core = lax.axis_index("core")
    base = (1 - core if flip else core) * (peers * rows)
    parts = sems.shape[0]
    span = peers // parts
    copies = []
    for part in range(parts):
        for p in range(part * span, (part + 1) * span):
            ends = widen(codes_ref[p, rows:, :])
            half_ref[pl.ds(p * rows, rows), :] = decode(widen(codes_ref[p, :rows, :]), ends[:SCALES])
        start = pl.multiple_of(base + part * span * rows, SUB)
        here = half_ref.at[pl.ds(part * span * rows, span * rows)]
        copies.append(pltpu.make_async_copy(here, out_hbm.at[pl.ds(start, span * rows)], sems.at[part]))
        copies[-1].start()
    for copy in copies:
        copy.wait()


def unpack(codes, table, before=None):
    peers, _, width = codes.shape
    hbm = pl.BlockSpec(memory_space=pltpu.HBM)
    flip = before is not None
    return pl.pallas_call(
        functools.partial(unpack_kernel, flip=flip),
        in_specs=[pl.BlockSpec(memory_space=pltpu.VMEM)] + [hbm] * flip,
        out_specs=hbm,
        out_shape=jax.ShapeDtypeStruct((table, width), jnp.float32),
        input_output_aliases={1: 0} if flip else {},
        scratch_shapes=[pltpu.VMEM((table // 2, width), jnp.float32), pltpu.SemaphoreType.DMA((math.gcd(peers, 4),))],
        cost_estimate=pl.CostEstimate(flops=table * width * 2, bytes_accessed=table * width * 3, transcendentals=0),
        compiler_params=ROOM,
        name="unpack",
    )(codes, *([before] if flip else []))


def partner(me, step, count):
    if count & (count - 1):
        return (me - step) % count, (me + step) % count
    return me ^ step, me ^ step


def cold_lots(owners):
    far, near = list(range(owners // 2, owners)), list(range(1, owners // 2))
    a, b, c = len(far) // 4, len(far) // 2, len(far) * 3 // 4
    return far[:a], far[a:b], far[b:c], near + far[c:]


def cold_kernel(got_ref, own_ref, *refs, block, at, lines, steps):
    moved, (out_ref, rhs_ref, row_ref) = refs[:-3], refs[-3:]
    owners, capacity, width = own_ref.shape
    half = out_ref.shape[0] // 2
    owner = lax.axis_index("gy")
    for step in range(owners):
        blocks = [ref for ref, n in zip(moved, steps) if n == step] or [own_ref.at[owner]]
        source, _ = partner(owner, step, owners)
        slots = got_ref[source, at:, :].astype(jnp.int32)[SCALES : SCALES + lines]
        high = (slots >= half).astype(jnp.int32)
        masked_halves((high == 0).astype(jnp.float32), blocks, rhs_ref, step * capacity, width)
        row_ref[pl.ds(step * lines, lines), :] = slots - high * half
    row = row_ref[...].astype(jnp.int16)
    rhs = rhs_ref[...]
    for start in range(0, half, block):
        part = jnp.dot(onehot_block(row, start, block), rhs, preferred_element_type=jnp.float32)
        out_ref[pl.ds(start, block), :] = part[:, :width]
        out_ref[pl.ds(half + start, block), :] = part[:, width:]


def cold_sums(got, own, moved, steps, table):
    owners, capacity, width = own.shape
    lines = capacity // LANES
    whole = pl.BlockSpec(memory_space=pltpu.VMEM)
    return pl.pallas_call(
        functools.partial(
            cold_kernel, block=math.gcd(table // 2, 256), at=got.shape[1] - tail_rows(lines), lines=lines, steps=steps
        ),
        in_specs=[whole] * (2 + len(moved)),
        out_specs=whole,
        out_shape=jax.ShapeDtypeStruct((table, width), jnp.float32),
        scratch_shapes=[
            pltpu.VMEM((owners * capacity, 2 * width), jnp.bfloat16),
            pltpu.VMEM((owners * lines, LANES), jnp.int32),
        ],
        cost_estimate=pl.CostEstimate(flops=2 * owners * capacity * table * width, bytes_accessed=2 * owners * capacity * width, transcendentals=0),
        compiler_params=ROOM,
        name="cold_sums",
    )(got, own, *moved)


def per_device(hot_ids, hot_grads, cold_grads, cold_slots, cold_counts):
    groups, owners = lax.axis_size("chip"), lax.axis_size("gy")
    peers = groups * owners
    everyone = ("chip", "gy")
    swap = [(0, 1), (1, 0)]
    factor = (HOT / (hot_ids.shape[0] * peers * 2)) ** 0.5

    capacity, width = cold_grads.shape[3:]
    lines = capacity // LANES
    blocks = cold_grads.reshape(owners, capacity, width)
    picked, moved = {}, []

    def take(*lots):
        steps = sorted({n for lot in lots for n in lot} - set(picked))
        if steps:
            picked.update(zip(steps, pick(blocks, steps)))

    def move(lot):
        for n in lot:
            pairs = [(i, partner(i, n, owners)[1]) for i in range(owners)]
            moved.append((n, lax.ppermute(picked[n], "gy", pairs)))

    early, middle, third, late = cold_lots(owners)
    take(early, middle)
    move(early)
    mine, send = hot_sums(hot_ids, hot_grads, HOT)
    got = lax.ppermute(send, "core", swap)
    move(middle)
    places = lax.broadcasted_iota(jnp.int32, (owners, capacity), 1)
    used = jnp.where(places < cold_counts.reshape(owners, 1), cold_slots.reshape(owners, capacity), -1)
    own, coded = pack(mine, got, groups, owners)
    crossed = []
    for n, block in enumerate(coded, 1):
        crossed.append(lax.ppermute(block, "chip", [(i, partner(i, n, groups)[1]) for i in range(groups)]))
    take(third, late)
    move(third)
    joined = join(own, used.reshape(owners, lines, LANES), crossed)
    parts = lax.all_to_all(joined, "gy", split_axis=0, concat_axis=0, tiled=True)
    move(late)
    summed = add(parts, factor, tail_rows(lines), peers)
    all_rows = lax.all_to_all(summed, everyone, split_axis=0, concat_axis=0, tiled=True)
    cold_grad = cold_sums(parts, blocks, [block for _, block in moved], [n for n, _ in moved], OWN_ROWS)
    others = lax.ppermute(all_rows, "core", swap)
    hot_half = unpack(all_rows, HOT)
    hot_grad = unpack(others, HOT, hot_half)
    return hot_grad, cold_grad.reshape(1, OWN_ROWS, width)


def solution(mesh):
    wide, owners = mesh.devices.shape
    split = Mesh(mesh.devices.reshape(wide // 2, 2, owners), ("chip", "core", "gy"))
    every = ("chip", "core", "gy")
    gx = ("chip", "core")
    return jax.shard_map(
        per_device,
        mesh=split,
        in_specs=(
            P(every),
            P(every, None),
            P(gx, "gy", None, None, None),
            P(gx, "gy", None, None),
            P(gx, "gy", None),
        ),
        out_specs=(P(), P(gx, "gy", None)),
        check_vma=False,
    )
```

```python
import functools
import math

import jax
import jax.numpy as jnp
from jax import lax
from jax.experimental import pallas as pl
from jax.experimental.pallas import tpu as pltpu
from jax.sharding import Mesh
from jax.sharding import PartitionSpec as P


HOT = 2048
OWN_ROWS = 2048
LANES = 128
SUB = 8
SCALES = SUB // 2
STEPS = 128.0
TOP = 32600.0
TINY = 2.0**-100
ROOM = pltpu.CompilerParams(vmem_limit_bytes=20 * 2**20)


def in_hbm(array):
    return pltpu.with_memory_space_constraint(array, pltpu.HBM)


def masked_halves(keep, data_refs, rhs_ref, base, width):
    flags = keep.T
    for j in range(keep.shape[0]):
        rows = pl.ds(base + j * LANES, LANES)
        column = jnp.broadcast_to(flags[:, j : j + 1], (LANES, width)).astype(jnp.bfloat16)
        data = sum(ref[pl.ds(j * LANES, LANES), :] for ref in data_refs)
        kept = data * column
        rhs_ref[rows, :width] = kept
        rhs_ref[rows, width:] = data - kept


def onehot_block(row, start, size):
    places = (lax.broadcasted_iota(jnp.int32, (size, LANES), 0) + start).astype(jnp.int16)
    one, zero = jnp.ones((), jnp.bfloat16), jnp.zeros((), jnp.bfloat16)
    parts = [jnp.where(places == row[j : j + 1, :], one, zero) for j in range(row.shape[0])]
    return jnp.concatenate(parts, axis=1)


def hot_kernel(ids_ref, data_ref, mine_ref, send_ref, rhs_ref, *, block, step):
    half, width = mine_ref.shape
    core = lax.axis_index("core")
    lines = step // LANES
    for first in range(0, data_ref.shape[0], step):
        ids = ids_ref[pl.ds(first // LANES, lines), :]
        high = (ids >= half).astype(jnp.int32)
        masked_halves((high == core).astype(jnp.float32), [data_ref.at[pl.ds(first, step)]], rhs_ref, 0, width)
        row = (ids - high * half).astype(jnp.int16)
        rhs = rhs_ref[...]
        for start in range(0, half, block):
            part = jnp.dot(onehot_block(row, start, block), rhs, preferred_element_type=jnp.float32)
            rows = pl.ds(start, block)
            if first == 0:
                mine_ref[rows, :] = part[:, :width]
                send_ref[rows, :] = part[:, width:]
            else:
                mine_ref[rows, :] += part[:, :width]
                send_ref[rows, :] += part[:, width:]


def hot_sums(ids, data, table):
    lookups, width = data.shape
    half = table // 2
    step = math.gcd(lookups, 8192)
    whole = pl.BlockSpec(memory_space=pltpu.VMEM)
    return pl.pallas_call(
        functools.partial(hot_kernel, block=math.gcd(half, 256), step=step),
        in_specs=[whole, whole],
        out_specs=[whole, whole],
        out_shape=[jax.ShapeDtypeStruct((half, width), jnp.float32)] * 2,
        scratch_shapes=[pltpu.VMEM((step, 2 * width), jnp.bfloat16)],
        cost_estimate=pl.CostEstimate(flops=2 * lookups * table * width, bytes_accessed=2 * lookups * width, transcendentals=0),
        compiler_params=ROOM,
        name="hot_sums",
    )(ids.reshape(lookups // LANES, LANES), data)


def pick_kernel(blocks_hbm, *refs, steps):
    outs, sems = refs[:-1], refs[-1]
    owner, owners = lax.axis_index("gy"), blocks_hbm.shape[0]
    copies = [
        pltpu.make_async_copy(blocks_hbm.at[partner(owner, step, owners)[1]], out, sems.at[n])
        for n, (step, out) in enumerate(zip(steps, outs))
    ]
    for copy in copies:
        copy.start()
    for copy in copies:
        copy.wait()


def pick(blocks, steps):
    count = len(steps)
    return pl.pallas_call(
        functools.partial(pick_kernel, steps=steps),
        in_specs=[pl.BlockSpec(memory_space=pltpu.HBM)],
        out_specs=[pl.BlockSpec(memory_space=pltpu.VMEM)] * count,
        out_shape=[jax.ShapeDtypeStruct(blocks.shape[1:], blocks.dtype)] * count,
        scratch_shapes=[pltpu.SemaphoreType.DMA((count,))],
        cost_estimate=pl.CostEstimate(flops=5 * 10**9, bytes_accessed=count * blocks[0].size * 2, transcendentals=0),
        compiler_params=ROOM,
        name="pick",
    )(in_hbm(blocks))


def encode(values):
    rows, width = values.shape
    groups = values.reshape(rows // SUB, SUB, width)
    most = jnp.max(jnp.abs(groups), axis=0)
    most = jnp.maximum(jnp.maximum(most[:SCALES], most[SCALES:]), TINY)
    code = jnp.ceil(jnp.log2(most) * STEPS) + 1.0
    scale = jnp.exp2(code * (-1.0 / STEPS)) * TOP
    codes = jnp.round(groups * jnp.concatenate([scale, scale], axis=0)[None])
    return codes.reshape(rows, width), code


def decode(codes, code):
    rows, width = codes.shape
    scale = jnp.exp2(code * (1.0 / STEPS)) * (1.0 / TOP)
    scale = jnp.concatenate([scale, scale], axis=0)
    return (codes.reshape(rows // SUB, SUB, width) * scale[None]).reshape(rows, width)


def narrow(values):
    return values.astype(jnp.int32).astype(jnp.int16)


def widen(values):
    return values.astype(jnp.int32).astype(jnp.float32)


def tail_rows(lines):
    return -(-(SCALES + lines) // SUB) * SUB


def pack_kernel(mine_ref, got_ref, own_ref, *out_refs):
    owners, rows, _ = out_refs[0].shape
    rows -= SUB
    groups = len(out_refs) + 1
    chip = lax.axis_index("chip")
    for step, out_ref in enumerate(out_refs, 1):
        base = partner(chip, step, groups)[1] * (owners * rows)
        for p in range(owners):
            here = pl.ds(pl.multiple_of(base + p * rows, SUB), rows)
            codes, code = encode(mine_ref[here, :] + got_ref[here, :])
            out_ref[p, :rows, :] = narrow(codes)
            out_ref[p, rows:, :] = narrow(jnp.concatenate([code, code], axis=0))
    here = pl.ds(pl.multiple_of(chip * (owners * rows), SUB), owners * rows)
    own_ref[...] = mine_ref[here, :] + got_ref[here, :]


def pack(mine, got, groups, owners):
    half, width = mine.shape
    rows = half // (groups * owners)
    whole = pl.BlockSpec(memory_space=pltpu.VMEM)
    own, *coded = pl.pallas_call(
        pack_kernel,
        in_specs=[whole, whole],
        out_specs=[whole] * groups,
        out_shape=[jax.ShapeDtypeStruct((owners * rows, width), jnp.float32)]
        + [jax.ShapeDtypeStruct((owners, rows + SUB, width), jnp.int16)] * (groups - 1),
        cost_estimate=pl.CostEstimate(flops=half * width * 8, bytes_accessed=half * width * 10, transcendentals=0),
        compiler_params=ROOM,
        name="pack",
    )(mine, got)
    return own, coded


def join_kernel(own_ref, slots_ref, *refs):
    got_refs, out_ref = refs[:-1], refs[-1]
    owners, lines, _ = slots_ref.shape
    tail = tail_rows(lines)
    rows = out_ref.shape[1] - tail
    spare = tail - SCALES - lines
    for p in range(owners):
        total = own_ref[p * rows : (p + 1) * rows, :]
        for ref in got_refs:
            ends = widen(ref[p, rows:, :])
            total += decode(widen(ref[p, :rows, :]), ends[:SCALES])
        codes, code = encode(total)
        out_ref[p, :rows, :] = narrow(codes)
        pieces = [code.astype(jnp.int32), slots_ref[p]]
        if spare:
            pieces.append(jnp.zeros((spare, LANES), jnp.int32))
        out_ref[p, rows:, :] = jnp.concatenate(pieces, axis=0).astype(jnp.int16)


def join(own, slots, got):
    owners, lines, _ = slots.shape
    total, width = own.shape
    whole = pl.BlockSpec(memory_space=pltpu.VMEM)
    return pl.pallas_call(
        join_kernel,
        in_specs=[whole] * (2 + len(got)),
        out_specs=whole,
        out_shape=jax.ShapeDtypeStruct((owners, total // owners + tail_rows(lines), width), jnp.int16),
        cost_estimate=pl.CostEstimate(flops=total * width * 8, bytes_accessed=total * width * 10, transcendentals=0),
        compiler_params=ROOM,
        name="join",
    )(own, slots, *got)


def add_kernel(got_ref, out_ref, *, factor, tail):
    peers, rows, width = got_ref.shape
    rows -= tail
    total = jnp.zeros((rows, width), jnp.float32)
    for p in range(peers):
        ends = widen(got_ref[p, rows:, :])
        total += decode(widen(got_ref[p, :rows, :]), ends[:SCALES])
    codes, code = encode(total * factor)
    body, ends = narrow(codes), narrow(jnp.concatenate([code, code], axis=0))
    for p in range(out_ref.shape[0]):
        out_ref[p, :rows, :] = body
        out_ref[p, rows:, :] = ends


def add(got, factor, tail, copies):
    _, rows, width = got.shape
    whole = pl.BlockSpec(memory_space=pltpu.VMEM)
    return pl.pallas_call(
        functools.partial(add_kernel, factor=factor, tail=tail),
        in_specs=[whole],
        out_specs=whole,
        out_shape=jax.ShapeDtypeStruct((copies, rows - tail + SUB, width), jnp.int16),
        cost_estimate=pl.CostEstimate(flops=got.size * 8, bytes_accessed=got.size * 4, transcendentals=0),
        compiler_params=ROOM,
        name="add",
    )(got)


def unpack_kernel(codes_ref, *refs, flip):
    out_hbm, half_ref, sems = refs[-3:]
    peers, rows, _ = codes_ref.shape
    rows -= SUB
    core = lax.axis_index("core")
    base = (1 - core if flip else core) * (peers * rows)
    parts = sems.shape[0]
    span = peers // parts
    copies = []
    for part in range(parts):
        for p in range(part * span, (part + 1) * span):
            ends = widen(codes_ref[p, rows:, :])
            half_ref[pl.ds(p * rows, rows), :] = decode(widen(codes_ref[p, :rows, :]), ends[:SCALES])
        start = pl.multiple_of(base + part * span * rows, SUB)
        here = half_ref.at[pl.ds(part * span * rows, span * rows)]
        copies.append(pltpu.make_async_copy(here, out_hbm.at[pl.ds(start, span * rows)], sems.at[part]))
        copies[-1].start()
    for copy in copies:
        copy.wait()


def unpack(codes, table, before=None):
    peers, _, width = codes.shape
    hbm = pl.BlockSpec(memory_space=pltpu.HBM)
    flip = before is not None
    return pl.pallas_call(
        functools.partial(unpack_kernel, flip=flip),
        in_specs=[pl.BlockSpec(memory_space=pltpu.VMEM)] + [hbm] * flip,
        out_specs=hbm,
        out_shape=jax.ShapeDtypeStruct((table, width), jnp.float32),
        input_output_aliases={1: 0} if flip else {},
        scratch_shapes=[pltpu.VMEM((table // 2, width), jnp.float32), pltpu.SemaphoreType.DMA((math.gcd(peers, 4),))],
        cost_estimate=pl.CostEstimate(flops=table * width * 2, bytes_accessed=table * width * 3, transcendentals=0),
        compiler_params=ROOM,
        name="unpack",
    )(codes, *([before] if flip else []))


def partner(me, step, count):
    if count & (count - 1):
        return (me - step) % count, (me + step) % count
    return me ^ step, me ^ step


def cold_lots(owners):
    far, near = list(range(owners // 2, owners)), list(range(1, owners // 2))
    a, b, c = len(far) // 4, len(far) // 2, len(far) * 3 // 4
    k = len(near) // 3
    return far[:a], far[a:b], far[b:c] + near[:k], near[k:] + far[c:]


def cold_kernel(got_ref, own_ref, *refs, block, at, lines, steps):
    moved, (out_ref, rhs_ref, row_ref) = refs[:-3], refs[-3:]
    owners, capacity, width = own_ref.shape
    half = out_ref.shape[0] // 2
    owner = lax.axis_index("gy")
    for step in range(owners):
        blocks = [ref for ref, n in zip(moved, steps) if n == step] or [own_ref.at[owner]]
        source, _ = partner(owner, step, owners)
        slots = got_ref[source, at:, :].astype(jnp.int32)[SCALES : SCALES + lines]
        high = (slots >= half).astype(jnp.int32)
        masked_halves((high == 0).astype(jnp.float32), blocks, rhs_ref, step * capacity, width)
        row_ref[pl.ds(step * lines, lines), :] = slots - high * half
    row = row_ref[...].astype(jnp.int16)
    rhs = rhs_ref[...]
    for start in range(0, half, block):
        part = jnp.dot(onehot_block(row, start, block), rhs, preferred_element_type=jnp.float32)
        out_ref[pl.ds(start, block), :] = part[:, :width]
        out_ref[pl.ds(half + start, block), :] = part[:, width:]


def cold_sums(got, own, moved, steps, table):
    owners, capacity, width = own.shape
    lines = capacity // LANES
    whole = pl.BlockSpec(memory_space=pltpu.VMEM)
    return pl.pallas_call(
        functools.partial(
            cold_kernel, block=math.gcd(table // 2, 256), at=got.shape[1] - tail_rows(lines), lines=lines, steps=steps
        ),
        in_specs=[whole] * (2 + len(moved)),
        out_specs=whole,
        out_shape=jax.ShapeDtypeStruct((table, width), jnp.float32),
        scratch_shapes=[
            pltpu.VMEM((owners * capacity, 2 * width), jnp.bfloat16),
            pltpu.VMEM((owners * lines, LANES), jnp.int32),
        ],
        cost_estimate=pl.CostEstimate(flops=2 * owners * capacity * table * width, bytes_accessed=2 * owners * capacity * width, transcendentals=0),
        compiler_params=ROOM,
        name="cold_sums",
    )(got, own, *moved)


def per_device(hot_ids, hot_grads, cold_grads, cold_slots, cold_counts):
    groups, owners = lax.axis_size("chip"), lax.axis_size("gy")
    peers = groups * owners
    everyone = ("chip", "gy")
    swap = [(0, 1), (1, 0)]
    factor = (HOT / (hot_ids.shape[0] * peers * 2)) ** 0.5

    capacity, width = cold_grads.shape[3:]
    lines = capacity // LANES
    blocks = cold_grads.reshape(owners, capacity, width)
    picked, moved = {}, []

    def take(*lots):
        steps = sorted({n for lot in lots for n in lot} - set(picked))
        if steps:
            picked.update(zip(steps, pick(blocks, steps)))

    def move(lot):
        for n in lot:
            pairs = [(i, partner(i, n, owners)[1]) for i in range(owners)]
            moved.append((n, lax.ppermute(picked[n], "gy", pairs)))

    early, middle, third, late = cold_lots(owners)
    take(early, middle)
    move(early)
    mine, send = hot_sums(hot_ids, hot_grads, HOT)
    got = lax.ppermute(send, "core", swap)
    move(middle)
    places = lax.broadcasted_iota(jnp.int32, (owners, capacity), 1)
    used = jnp.where(places < cold_counts.reshape(owners, 1), cold_slots.reshape(owners, capacity), -1)
    own, coded = pack(mine, got, groups, owners)
    crossed = []
    for n, block in enumerate(coded, 1):
        crossed.append(lax.ppermute(block, "chip", [(i, partner(i, n, groups)[1]) for i in range(groups)]))
    take(third, late)
    move(third)
    joined = join(own, used.reshape(owners, lines, LANES), crossed)
    parts = lax.all_to_all(joined, "gy", split_axis=0, concat_axis=0, tiled=True)
    move(late)
    summed = add(parts, factor, tail_rows(lines), peers)
    all_rows = lax.all_to_all(summed, everyone, split_axis=0, concat_axis=0, tiled=True)
    cold_grad = cold_sums(parts, blocks, [block for _, block in moved], [n for n, _ in moved], OWN_ROWS)
    others = lax.ppermute(all_rows, "core", swap)
    hot_half = unpack(all_rows, HOT)
    hot_grad = unpack(others, HOT, hot_half)
    return hot_grad, cold_grad.reshape(1, OWN_ROWS, width)


def solution(mesh):
    wide, owners = mesh.devices.shape
    split = Mesh(mesh.devices.reshape(wide // 2, 2, owners), ("chip", "core", "gy"))
    every = ("chip", "core", "gy")
    gx = ("chip", "core")
    return jax.shard_map(
        per_device,
        mesh=split,
        in_specs=(
            P(every),
            P(every, None),
            P(gx, "gy", None, None, None),
            P(gx, "gy", None, None),
            P(gx, "gy", None),
        ),
        out_specs=(P(), P(gx, "gy", None)),
        check_vma=False,
    )
```
